32 devices in a mesh: gx: 8 (over z, core), gy: 4 (over y, x).
Axes of the slice: x: 2, y: 2, z: 4, core: 2. Of those that a mesh axis runs over, the one named last changes fastest.
Arguments:
- density: float32 [256, 256, 256], P('gx', 'gy'), may hold values from 0.05 to 2
Outputs:
- potential: float32 [256, 256, 256], P('gx', 'gy')
- energy: float32 [], replicated
The draws below stay inside these ranges and needn't reach their ends.
All inputs are finite; a program needn't handle non-finite values.
Results may differ from the reference program's by a relative error of at most 0.00005.
Values sent between devices are 32-bit elements.
A program may use at most 128 MiB of HBM per device.

```python
import math
import jax
import jax.numpy as jnp

NX = 256
NY = 256
NZ = 256


def block_scale(stream_key, dims, split, least, high):
    gain = 1.0
    for position, blocks in split:
        heights = jax.random.uniform(jax.random.fold_in(jax.random.fold_in(stream_key, 6), position), (blocks,), jnp.float32, least / len(split), high / len(split))
        gain = gain * jnp.repeat(jnp.exp(heights), dims[position] // blocks).reshape((-1,) + (1,) * (len(dims) - 1 - position))
    return gain


def setup_inputs(seed: int = 0) -> dict:
    streams_of = jax.random.split(jax.random.key(seed), 2)
    density = jnp.clip(jnp.exp(math.log(2.0) - 3.6888794 * jax.random.uniform(streams_of[0], (NX, NY, NZ), jnp.float32) ** block_scale(streams_of[0], (NX, NY, NZ), ((0, 8), (1, 4)), -0.2, 0.2)), 0.05, 2.0)
    return dict(density=density)


spacing = 1.0
pbe_kappa = 0.804
pbe_mu = 0.2195149727645171
pbe_beta = 0.06672455060314922
pbe_gamma = 0.031090690869654894
pw_coef = 0.0310907
pw_alpha = 0.2137
pw_first = 7.5957
pw_second = 3.5876
pw_third = 1.6382
pw_fourth = 0.49294

def xc_energy(electrons, grad_sq):
    k_fermi = jnp.cbrt(3.0 * math.pi ** 2 * electrons)
    exch_unif = -0.75 * k_fermi / math.pi
    s_square = grad_sq / (4.0 * k_fermi ** 2 * electrons ** 2)
    enhance = 1.0 + pbe_kappa - pbe_kappa / (1.0 + pbe_mu * s_square / pbe_kappa)
    wigner = jnp.cbrt(3.0 / (4.0 * math.pi * electrons))
    root_rs = jnp.sqrt(wigner)
    series = 2.0 * pw_coef * (pw_first * root_rs + pw_second * wigner + pw_third * wigner * root_rs + pw_fourth * wigner ** 2)
    corr_unif = -2.0 * pw_coef * (1.0 + pw_alpha * wigner) * jnp.log(1.0 + 1.0 / series)
    screen_sq = 4.0 * k_fermi / math.pi
    t_square = grad_sq / (4.0 * screen_sq * electrons ** 2)
    factor = pbe_beta / pbe_gamma / jnp.expm1(-corr_unif / pbe_gamma)
    scaled = factor * t_square
    gradient_term = pbe_gamma * jnp.log(1.0 + pbe_beta / pbe_gamma * t_square * (1.0 + scaled) / (1.0 + scaled + scaled ** 2))
    return electrons * (exch_unif * enhance + corr_unif + gradient_term)

def summed_energy(electrons, grad_sq):
    return jnp.sum(xc_energy(electrons, grad_sq))

def wavenum(count):
    index = jnp.arange(count, dtype=jnp.int32)
    signed = jnp.where(index < count // 2, index, index - count)
    signed = jnp.where(index == count // 2, 0, signed)
    return signed.astype(jnp.float32) * (2.0 * math.pi / (count * spacing))

def reference(density):
    spectrum = jnp.fft.fftn(density)
    waves = (wavenum(NX)[:, None, None], wavenum(NY)[None, :, None], wavenum(NZ)[None, None, :])
    gradients = [jnp.real(jnp.fft.ifftn(1j * wavevec * spectrum)) for wavevec in waves]
    grad_sq = gradients[0] ** 2 + gradients[1] ** 2 + gradients[2] ** 2
    energy_sum, partials = jax.value_and_grad(summed_energy, argnums=(0, 1))(density, grad_sq)
    d_dens, d_grad = partials
    flux_spec = 1j * waves[0] * jnp.fft.fftn(2.0 * d_grad * gradients[0])
    flux_spec = flux_spec + 1j * waves[1] * jnp.fft.fftn(2.0 * d_grad * gradients[1])
    flux_spec = flux_spec + 1j * waves[2] * jnp.fft.fftn(2.0 * d_grad * gradients[2])
    divergence = jnp.real(jnp.fft.ifftn(flux_spec))
    potential = d_dens - divergence
    energy = energy_sum / (NX * NY * NZ)
    return (potential, energy)
```

```python
import functools
import math

import jax
import jax.numpy as jnp
import numpy as np
from jax import lax
from jax.experimental import pallas as pl
from jax.experimental.pallas import tpu as pltpu
from jax.sharding import PartitionSpec as P

spacing = 1.0
highest = lax.Precision.HIGHEST
pbe_kappa = 0.804
pbe_mu = 0.2195149727645171
pbe_beta = 0.06672455060314922
pbe_gamma = 0.031090690869654894
pw_coef = 0.0310907
pw_alpha = 0.2137
pw_first = 7.5957
pw_second = 3.5876
pw_third = 1.6382
pw_fourth = 0.49294


def xc_energy(electrons, grad_sq):
    third = jnp.exp(jnp.log(electrons) * (1.0 / 3.0))
    k_fermi = (3.0 * math.pi**2) ** (1.0 / 3.0) * third
    exch_unif = -0.75 / math.pi * k_fermi
    inv_sq = grad_sq / (4.0 * k_fermi * electrons * electrons)
    s_square = inv_sq / k_fermi
    enhance = 1.0 + pbe_kappa - pbe_kappa / (1.0 + (pbe_mu / pbe_kappa) * s_square)
    wigner = (3.0 / (4.0 * math.pi)) ** (1.0 / 3.0) / third
    root_rs = jnp.sqrt(wigner)
    series = (
        2.0
        * pw_coef
        * root_rs
        * (pw_first + root_rs * (pw_second + root_rs * (pw_third + root_rs * pw_fourth)))
    )
    corr_unif = -2.0 * pw_coef * (1.0 + pw_alpha * wigner) * jnp.log(1.0 + 1.0 / series)
    t_square = inv_sq * (math.pi / 4.0)
    factor = (pbe_beta / pbe_gamma) / (jnp.exp(corr_unif * (-1.0 / pbe_gamma)) - 1.0)
    scaled = factor * t_square
    gradient_term = pbe_gamma * jnp.log(
        1.0 + (pbe_beta / pbe_gamma) * t_square * (1.0 + scaled) / (1.0 + scaled + scaled * scaled)
    )
    return electrons * (exch_unif * enhance + corr_unif + gradient_term)


def deriv_matrix(count):
    positions = np.arange(count)
    signed = np.where(positions < count // 2, positions, positions - count)
    signed = np.where(positions == count // 2, 0, signed)
    waves = signed * (2.0 * math.pi / (count * spacing))
    phase = (positions[:, None] * positions[None, :] % count) * (2.0 * math.pi / count)
    cosine, sine = np.cos(phase), np.sin(phase)
    first = (cosine.T * waves[None, :]) @ sine
    second = (sine.T * waves[None, :]) @ cosine
    return ((first - second) / count).astype(np.float32)


def far_first(count):
    return sorted(range(1, count), key=lambda k: abs(2 * k - count))


def kernel(
    num_gx, num_gy, zc,
    n_hbm, dmx_hbm, dmy_hbm, dmz_hbm,
    out_ref, energy_ref,
    n_ref, dmx_ref, dmy_ref, dmz_ref,
    n_t, lx1, rx1, gx_t, gx, ly1, ry1, gy, gz, fx_t, lx2, rx2, dx_t, ly2, ry2, dy,
    acc, part_y, tot_y, part_x,
    xs_sem, xr_sem, ys_sem, yr_sem, es_sem, er_sem, in_sem,
):
    rows_x, rows_y, count_z = n_ref.shape
    block_y = rows_y // num_gx
    block_x = rows_x // num_gy
    count_x = rows_x * num_gx
    count_y = rows_y * num_gy
    chunks = count_z // zc
    me_x = lax.axis_index("gx")
    me_y = lax.axis_index("gy")

    def peer_x(k):
        return lax.rem(me_x + k, num_gx)

    def peer_y(k):
        return lax.rem(me_y + k, num_gy)

    def zs(c):
        return pl.ds(c * zc, zc)

    def x_block(i):
        return pl.ds(i * block_y, block_y)

    def x_rows(i):
        return pl.ds(pl.multiple_of(i * rows_x, rows_x), rows_x)

    def y_block(i):
        return pl.ds(i * block_x, block_x)

    def y_rows(i):
        return pl.ds(pl.multiple_of(i * rows_y, rows_y), rows_y)

    loads = [
        pltpu.make_async_copy(n_hbm.at[:, :, zs(c)], n_ref.at[:, :, zs(c)], in_sem.at[c])
        for c in range(chunks)
    ]
    pairs = ((dmz_hbm, dmz_ref), (dmy_hbm, dmy_ref), (dmx_hbm, dmx_ref))
    tables = [
        pltpu.make_async_copy(source, target, in_sem.at[chunks + place])
        for place, (source, target) in enumerate(pairs)
    ]
    for copy in loads + tables:
        copy.start()
    barrier = pltpu.get_barrier_semaphore()
    for k in range(1, num_gx):
        pl.semaphore_signal(
            barrier, inc=1, device_id={"gx": peer_x(k)}, device_id_type=pl.DeviceIdType.MESH
        )
    for k in range(1, num_gy):
        pl.semaphore_signal(
            barrier, inc=1, device_id={"gy": peer_y(k)}, device_id_type=pl.DeviceIdType.MESH
        )
    def send_x(phase, c, source, target, forward):
        copies = []
        for k in far_first(num_gx):
            to = peer_x(k)
            if forward:
                src, dst = source.at[x_block(to), :, zs(c)], target.at[:, x_rows(me_x), zs(c)]
            else:
                src, dst = source.at[:, x_rows(to), zs(c)], target.at[x_block(me_x), :, zs(c)]
            copy = pltpu.make_async_remote_copy(
                src_ref=src, dst_ref=dst,
                send_sem=xs_sem.at[phase, c, k], recv_sem=xr_sem.at[phase, c, k],
                device_id={"gx": to}, device_id_type=pl.DeviceIdType.MESH,
            )
            copy.start()
            copies.append(copy)
        if forward:
            target[:, x_rows(me_x), zs(c)] = source[x_block(me_x), :, zs(c)]
        else:
            target[x_block(me_x), :, zs(c)] = source[:, x_rows(me_x), zs(c)]
        return copies

    def send_y(phase, c, source, target, forward):
        copies = []
        for k in far_first(num_gy):
            to = peer_y(k)
            if forward:
                src, dst = source.at[y_block(to), :, zs(c)], target.at[:, y_rows(me_y), zs(c)]
            else:
                src, dst = source.at[:, y_rows(to), zs(c)], target.at[y_block(me_y), :, zs(c)]
            copy = pltpu.make_async_remote_copy(
                src_ref=src, dst_ref=dst,
                send_sem=ys_sem.at[phase, c, k], recv_sem=yr_sem.at[phase, c, k],
                device_id={"gy": to}, device_id_type=pl.DeviceIdType.MESH,
            )
            copy.start()
            copies.append(copy)
        if forward:
            target[:, y_rows(me_y), zs(c)] = source[y_block(me_y), :, zs(c)]
        else:
            target[y_block(me_y), :, zs(c)] = source[:, y_rows(me_y), zs(c)]
        return copies

    def arrived(copies):
        for copy in copies:
            copy.wait_recv()

    def lines(matrix, source, target, c):
        @pl.loop(0, source.shape[0])
        def _(i):
            target[i, :, zs(c)] = jnp.dot(
                matrix[...], source[i, :, zs(c)],
                precision=highest, preferred_element_type=jnp.float32,
            )

    step = min(8, rows_y)

    def turn_in(source, target, c):
        @pl.loop(0, rows_y // step)
        def _(j):
            y0 = pl.multiple_of(j * step, step)
            target[pl.ds(y0, step), :, zs(c)] = jnp.swapaxes(
                source[:, pl.ds(y0, step), zs(c)], 0, 1
            )

    def turn_out(source, target, c):
        @pl.loop(0, rows_y // step)
        def _(j):
            y0 = pl.multiple_of(j * step, step)
            target[:, pl.ds(y0, step), zs(c)] = jnp.swapaxes(
                source[pl.ds(y0, step), :, zs(c)], 0, 1
            )

    group = min(rows_x, max(1, 256 // rows_y))

    def along_z(source):
        def at(i):
            return pl.ds(i * group, group)

        def product(i):
            flat = source[at(i)].reshape(group * rows_y, count_z)
            result = jnp.dot(
                flat, dmz_ref[...], precision=highest, preferred_element_type=jnp.float32
            )
            return result.reshape(group, rows_y, count_z)

        return at, product

    sent = []
    every = range(chunks)
    fy1, fx1 = [], []
    for c in every:
        loads[c].wait()
        turn_in(n_ref, n_t, c)
        if c == 0:
            pl.semaphore_wait(barrier, num_gx + num_gy - 2)
        fx1.append(send_x(0, c, n_t, lx1, True))
        fy1.append(send_y(0, c, n_ref, ly1, True))
    for copy in tables:
        copy.wait()
    at, product = along_z(n_ref)

    @pl.loop(0, rows_x // group)
    def _(i):
        gz[at(i)] = product(i)

    by1, bx1 = [], []
    for c in every:
        arrived(fy1[c])
        lines(dmy_ref, ly1, ry1, c)
        by1.append(send_y(1, c, ry1, gy, False))
    for c in every:
        arrived(fx1[c])
        lines(dmx_ref, lx1, rx1, c)
        bx1.append(send_x(1, c, rx1, gx_t, False))

    acc[...] = jnp.zeros_like(acc)
    part = min(rows_y, 32)
    fx2, fy2 = [], []
    for c in every:
        arrived(by1[c])
        arrived(bx1[c])
        turn_out(gx_t, gx, c)

        @pl.loop(0, rows_x)
        def _(i):
            @pl.loop(0, rows_y // part)
            def _(j):
                where = (i, pl.ds(pl.multiple_of(j * part, part), part), zs(c))
                dens, grad_x, grad_y, grad_z = n_ref[where], gx[where], gy[where], gz[where]
                grad_sq = grad_x * grad_x + grad_y * grad_y + grad_z * grad_z
                value, pull = jax.vjp(xc_energy, dens, grad_sq)
                d_dens, d_grad = pull(jnp.ones_like(value))
                twice = 2.0 * d_grad
                out_ref[where] = d_dens
                gx[where] = twice * grad_x
                gy[where] = twice * grad_y
                gz[where] = twice * grad_z
                acc[...] += value

        turn_in(gx, fx_t, c)
        fx2.append(send_x(2, c, fx_t, lx2, True))
        fy2.append(send_y(2, c, gy, ly2, True))

    energy = jnp.sum(acc[...].reshape(-1, 8, zc), axis=0)
    part_y[me_y] = energy
    energy_copies = []
    for k in range(1, num_gy):
        copy = pltpu.make_async_remote_copy(
            src_ref=part_y.at[me_y], dst_ref=part_y.at[me_y],
            send_sem=es_sem.at[0, k], recv_sem=er_sem.at[0, k],
            device_id={"gy": peer_y(k)}, device_id_type=pl.DeviceIdType.MESH,
        )
        copy.start()
        energy_copies.append(copy)

    at, product = along_z(gz)

    @pl.loop(0, rows_x // group)
    def _(i):
        out_ref[at(i)] = out_ref[at(i)] - product(i)

    arrived(energy_copies)
    sent.append(energy_copies)
    tot_y[...] = jnp.sum(part_y[...], axis=0)
    part_x[me_x] = tot_y[...]
    energy_copies = []
    for k in range(1, num_gx):
        copy = pltpu.make_async_remote_copy(
            src_ref=tot_y, dst_ref=part_x.at[me_x],
            send_sem=es_sem.at[1, k], recv_sem=er_sem.at[1, k],
            device_id={"gx": peer_x(k)}, device_id_type=pl.DeviceIdType.MESH,
        )
        copy.start()
        energy_copies.append(copy)

    bx2, by2 = [], []
    for c in every:
        arrived(fy2[c])
        lines(dmy_ref, ly2, ry2, c)
        by2.append(send_y(3, c, ry2, dy, False))
        arrived(fx2[c])
        lines(dmx_ref, lx2, rx2, c)
        bx2.append(send_x(3, c, rx2, dx_t, False))

    arrived(energy_copies)
    sent.append(energy_copies)
    cells = float(count_x * count_y * count_z)
    total = jnp.sum(part_x[...], axis=0)
    energy_ref[...] = jnp.sum(total, axis=(0, 1), keepdims=True) * (1.0 / cells)

    for c in every:
        arrived(by2[c])
        arrived(bx2[c])

        @pl.loop(0, rows_y // step)
        def _(j):
            y0 = pl.multiple_of(j * step, step)
            where = (slice(None), pl.ds(y0, step), zs(c))
            turned = jnp.swapaxes(dx_t[pl.ds(y0, step), :, zs(c)], 0, 1)
            out_ref[where] = out_ref[where] - (dy[where] + turned)

    for copies in sent + fx1 + fy1 + bx1 + by1 + fx2 + fy2 + bx2 + by2:
        for copy in copies:
            copy.wait_send()


def chip_kernel(
    num_gx, num_gy, parts,
    n_hbm, dmx_hbm, dmy_hbm, dmz_hbm,
    out_ref, energy_ref,
    n_ref, dmx_ref, dmy_ref, dmz_ref,
    n_t, n_lines, g_lines, gx_t, gx, fx_t, f_lines, dx_t,
    ly1, ly2, ry, gy, dy, gz,
    far_n, far_ly, far_ry, far_gy, far_other, far_gz,
    acc, part_y, tot_y, part_x,
    ns_sem, nr_sem, gs_sem, gr_sem, fs_sem, fr_sem, ds_sem, dr_sem,
    ys_sem, yr_sem, ws_sem, wr_sem, os_sem, or_sem, es_sem, er_sem, in_sem,
):
    rows_x, rows_y, count_z = n_ref.shape
    half = count_z // 2
    chip_x = 2 * rows_x
    block_x = rows_x // num_gy
    far_block = chip_x // num_gy
    count_x = rows_x * num_gx
    count_y = rows_y * num_gy
    span = rows_y // parts
    me_x = lax.axis_index("gx")
    me_y = lax.axis_index("gy")
    core = lax.rem(me_x, 2)
    chip = me_x // 2
    chips = num_gx // 2
    is_inner = jnp.logical_and(chip > 0, chip < chips - 1)
    low = chip < 2
    inner = jnp.where(low, 1, 2)
    outer = jnp.where(low, 0, 3)
    opposite = 3 - inner
    far_outer = 3 - outer
    mate = chip * 2 + (1 - core)
    every = range(parts)
    lanes_count = 2

    def zs(c):
        if isinstance(c, int):
            return pl.ds(c * half, half)
        return pl.ds(pl.multiple_of(c * half, half), half)

    def ys(s):
        return pl.ds(s * span, span)

    def x_rows(device):
        return pl.ds(pl.multiple_of(device * rows_x, rows_x), rows_x)

    def chip_rows(which):
        return pl.ds(pl.multiple_of(which * chip_x, chip_x), chip_x)

    def local_rows(start, size):
        return pl.ds(pl.multiple_of(start, rows_x), size)

    def peer_y(k):
        return lax.rem(me_y + k, num_gy)

    def y_rows(i):
        return pl.ds(pl.multiple_of(i * rows_y, rows_y), rows_y)

    def to_x(device, source, target, send, recv):
        return pltpu.make_async_remote_copy(
            src_ref=source, dst_ref=target, send_sem=send, recv_sem=recv,
            device_id={"gx": device}, device_id_type=pl.DeviceIdType.MESH,
        )

    def landed(target, recv):
        to_x(mate, target, target, recv, recv).wait_recv()

    loads = [
        pltpu.make_async_copy(n_hbm.at[:, :, zs(c)], n_ref.at[:, :, zs(c)], in_sem.at[c])
        for c in range(lanes_count)
    ]
    pairs = ((dmz_hbm, dmz_ref), (dmy_hbm, dmy_ref), (dmx_hbm, dmx_ref))
    tables = [
        pltpu.make_async_copy(source, target, in_sem.at[lanes_count + place])
        for place, (source, target) in enumerate(pairs)
    ]
    for copy in loads + tables:
        copy.start()
    barrier = pltpu.get_barrier_semaphore()
    for k in range(1, num_gx):
        pl.semaphore_signal(
            barrier, inc=1, device_id={"gx": lax.rem(me_x + k, num_gx)},
            device_id_type=pl.DeviceIdType.MESH,
        )
    for k in range(1, num_gy):
        pl.semaphore_signal(
            barrier, inc=1, device_id={"gy": peer_y(k)}, device_id_type=pl.DeviceIdType.MESH
        )

    def y_copies(phase, c, source, target, forward):
        copies = []
        for k in far_first(num_gy):
            to = peer_y(k)
            theirs, mine = pl.ds(to * block_x, block_x), pl.ds(me_y * block_x, block_x)
            if forward:
                src, dst = source.at[theirs, :, zs(c)], target.at[:, y_rows(me_y), zs(c)]
            else:
                src, dst = source.at[:, y_rows(to), zs(c)], target.at[mine, :, zs(c)]
            copies.append(pltpu.make_async_remote_copy(
                src_ref=src, dst_ref=dst,
                send_sem=ys_sem.at[phase, c, k], recv_sem=yr_sem.at[phase, c, k],
                device_id={"gy": to}, device_id_type=pl.DeviceIdType.MESH,
            ))
        return copies

    y_plan = ((n_ref, ly1, True), (ry, gy, False), (gy, ly2, True), (ry, dy, False))

    def y_send(phase, c):
        source, target, forward = y_plan[phase]
        for copy in y_copies(phase, c, source, target, forward):
            copy.start()
        mine = pl.ds(me_y * block_x, block_x)
        if forward:
            target[:, y_rows(me_y), zs(c)] = source[mine, :, zs(c)]
        else:
            target[mine, :, zs(c)] = source[:, y_rows(me_y), zs(c)]

    def y_wait(phase, c, sent):
        for copy in y_copies(phase, c, *y_plan[phase]):
            if sent:
                copy.wait_send()
            else:
                copy.wait_recv()

    def far_copies(phase):
        copies = []
        for k in far_first(num_gy):
            to = peer_y(k)
            if phase == 0:
                src = far_n.at[pl.ds(to * far_block, far_block)]
                dst = far_ly.at[:, y_rows(me_y), :]
            else:
                src = far_ry.at[:, y_rows(to), :]
                dst = far_gy.at[pl.ds(me_y * far_block, far_block)]
            copies.append(pltpu.make_async_remote_copy(
                src_ref=src, dst_ref=dst,
                send_sem=ws_sem.at[phase, k], recv_sem=wr_sem.at[phase, k],
                device_id={"gy": to}, device_id_type=pl.DeviceIdType.MESH,
            ))
        return copies

    def far_send(phase):
        for copy in far_copies(phase):
            copy.start()
        mine = pl.ds(me_y * far_block, far_block)
        if phase == 0:
            far_ly[:, y_rows(me_y), :] = far_n[mine]
        else:
            far_gy[mine] = far_ry[:, y_rows(me_y), :]

    def far_wait(phase, sent):
        for copy in far_copies(phase):
            if sent:
                copy.wait_send()
            else:
                copy.wait_recv()

    def product(left, right):
        return jnp.dot(left, right, precision=highest, preferred_element_type=jnp.float32)

    def y_lines(source, c):
        @pl.loop(0, block_x)
        def _(i):
            ry[i, :, zs(c)] = product(dmy_ref[...], source[i, :, zs(c)])

    group = min(rows_x, max(1, 256 // rows_y))

    def along_z(source, i):
        flat = source[pl.ds(i * group, group)].reshape(group * rows_y, count_z)
        return product(flat, dmz_ref[...]).reshape(group, rows_y, count_z)

    step = min(8, span)

    def turned(source, target, s):
        @pl.loop(0, span // step)
        def _(j):
            y0 = pl.multiple_of(s * span + j * step, step)
            target[pl.ds(y0, step)] = jnp.swapaxes(source[:, pl.ds(y0, step), :], 0, 1)

    def n_sends(s, role):
        copies = []
        if role == "outer":
            for j in range(2):
                copies.append(to_x(
                    inner * 2 + j, n_t.at[ys(s), :, zs(j)], n_lines.at[ys(s), x_rows(me_x), :],
                    ns_sem.at[j, s], nr_sem.at[core, s],
                ))
        else:
            for j in range(2):
                copies.append(to_x(
                    opposite * 2 + j, n_t.at[ys(s), :, zs(j)], n_lines.at[ys(s), x_rows(me_x), :],
                    ns_sem.at[j, s], nr_sem.at[2 + core, s],
                ))
            copies.append(to_x(
                mate, n_t.at[ys(s), :, zs(1 - core)], n_lines.at[ys(s), x_rows(me_x), :],
                ns_sem.at[2, s], nr_sem.at[4, s],
            ))
        return copies

    def forward_copy(lines, send, recv, s):
        part = lines.at[ys(s), chip_rows(outer), :]
        return to_x(opposite * 2 + core, part, part, send.at[3, s], recv.at[5, s])

    def from_outer(lines, recv, s):
        for j in range(2):
            landed(lines.at[ys(s), x_rows(outer * 2 + j), :], recv.at[j, s])

    def f_sends(s, role):
        copies = []
        if role == "outer":
            for j in range(2):
                copies.append(to_x(
                    inner * 2 + j, fx_t.at[ys(s), :, zs(j)], f_lines.at[ys(s), x_rows(me_x), :],
                    fs_sem.at[j, s], fr_sem.at[core, s],
                ))
        else:
            copies.append(to_x(
                mate, fx_t.at[ys(s), :, zs(1 - core)], f_lines.at[ys(s), x_rows(me_x), :],
                fs_sem.at[2, s], fr_sem.at[4, s],
            ))
        return copies

    def back_copies(own, other, target, send, recv, s):
        copies = []
        for j in range(2):
            copies.append(to_x(
                outer * 2 + j, g_lines.at[ys(s), local_rows(other + j * rows_x, rows_x), :],
                target.at[ys(s), :, zs(core)], send.at[j, s], recv.at[core, s],
            ))
        copies.append(to_x(
            mate, g_lines.at[ys(s), local_rows(own + (1 - core) * rows_x, rows_x), :],
            target.at[ys(s), :, zs(core)], send.at[2, s], recv.at[core, s],
        ))
        return copies

    first_own, first_other, first_far = chip_x, jnp.where(low, 0, 2 * chip_x), jnp.where(low, 2 * chip_x, 0)
    second_own, second_other = jnp.where(low, chip_x, 0), jnp.where(low, 0, chip_x)

    def x_back(own, other, target, send, recv, s):
        for copy in back_copies(own, other, target, send, recv, s):
            copy.start()
        target[ys(s), :, zs(core)] = g_lines[ys(s), local_rows(own + core * rows_x, rows_x), :]

    def x_lines(source, first_row, rows, s):
        @pl.loop(0, span)
        def _(j):
            y = s * span + j
            matrix = dmx_ref[pl.ds(pl.multiple_of(first_row, chip_x), rows), :]
            g_lines[y, pl.ds(0, rows), :] = product(matrix, source[y])

    deep = min(rows_x, max(1, 32 // (span * lanes_count)))

    def pointwise(s):
        @pl.loop(0, span // step)
        def _(j):
            y0 = pl.multiple_of(s * span + j * step, step)
            gx[:, pl.ds(y0, step), :] = jnp.swapaxes(gx_t[pl.ds(y0, step)], 0, 1)

        @pl.loop(0, rows_x // deep)
        def _(i):
            where = (pl.ds(i * deep, deep), ys(s))
            dens, grad_x, grad_y, grad_z = n_ref[where], gx[where], gy[where], gz[where]
            grad_sq = grad_x * grad_x + grad_y * grad_y + grad_z * grad_z
            value, pull = jax.vjp(xc_energy, dens, grad_sq)
            d_dens, d_grad = pull(jnp.ones_like(value))
            twice = 2.0 * d_grad
            out_ref[where] = d_dens
            gx[where] = twice * grad_x
            gy[where] = twice * grad_y
            gz[where] = twice * grad_z
            acc[...] += value

        turned(gx, fx_t, s)

    def z_gradient():
        @pl.loop(0, rows_x // group)
        def _(i):
            gz[pl.ds(i * group, group)] = along_z(n_ref, i)

    def z_divergence():
        @pl.loop(0, rows_x // group)
        def _(i):
            at = pl.ds(i * group, group)
            out_ref[at] = out_ref[at] - along_z(gz, i)

    def energy_copies(phase):
        copies = []
        count = num_gy if phase == 0 else num_gx
        for k in range(1, count):
            if phase == 0:
                to, src, dst = {"gy": peer_y(k)}, part_y.at[me_y], part_y.at[me_y]
            else:
                to, src, dst = {"gx": lax.rem(me_x + k, num_gx)}, tot_y, part_x.at[me_x]
            copies.append(pltpu.make_async_remote_copy(
                src_ref=src, dst_ref=dst,
                send_sem=es_sem.at[phase, k], recv_sem=er_sem.at[phase, k],
                device_id=to, device_id_type=pl.DeviceIdType.MESH,
            ))
        return copies

    def energy_first():
        total = jnp.sum(acc[...].reshape(-1, 8, count_z), axis=0)
        part_y[me_y] = total[:, :half] + total[:, half:]
        for copy in energy_copies(0):
            copy.start()

    def energy_second():
        for copy in energy_copies(0):
            copy.wait_recv()
        tot_y[...] = jnp.sum(part_y[...], axis=0)
        part_x[me_x] = tot_y[...]
        for copy in energy_copies(1):
            copy.start()

    def energy_last():
        for copy in energy_copies(1):
            copy.wait_recv()
        cells = float(count_x * count_y * count_z)
        total = jnp.sum(part_x[...], axis=0)
        energy_ref[...] = jnp.sum(total, axis=(0, 1), keepdims=True) * (1.0 / cells)

    def finish(s, sources):
        for j in sources:
            landed(dx_t.at[ys(s), :, zs(j)], dr_sem.at[j, s])

        @pl.loop(0, span // step)
        def _(j):
            y0 = pl.multiple_of(s * span + j * step, step)
            where = (slice(None), pl.ds(y0, step))
            side = jnp.swapaxes(dx_t[pl.ds(y0, step)], 0, 1)
            out_ref[where] = out_ref[where] - (dy[where] + side)

    def start_n(role):
        for s in every:
            turned(n_ref, n_t, s)
            for copy in n_sends(s, role):
                copy.start()
            if role == "inner":
                n_lines[ys(s), x_rows(me_x), :] = n_t[ys(s), :, zs(core)]

    def y_first(c):
        y_wait(0, c, False)
        y_lines(ly1, c)
        y_send(1, c)

    def y_second(c):
        y_wait(2, c, False)
        if c == 0:
            for other in range(lanes_count):
                y_wait(1, other, True)
        y_lines(ly2, c)
        y_send(3, c)

    acc[...] = jnp.zeros_like(acc)
    for c in range(lanes_count):
        loads[c].wait()
        if c == 0:
            pl.semaphore_wait(barrier, num_gx + num_gy - 2)
        y_send(0, c)

    def outer_program():
        start_n("outer")
        for copy in tables:
            copy.wait()
        z_gradient()
        for c in range(lanes_count):
            y_first(c)
        for c in range(lanes_count):
            y_wait(1, c, False)
        for s in every:
            for j in range(2):
                landed(gx_t.at[ys(s), :, zs(j)], gr_sem.at[j, s])
            pointwise(s)
            for copy in f_sends(s, "outer"):
                copy.start()
        for c in range(lanes_count):
            y_send(2, c)
        energy_first()
        z_divergence()
        energy_second()
        for c in range(lanes_count):
            y_second(c)
        energy_last()
        for c in range(lanes_count):
            y_wait(3, c, False)
        for s in every:
            finish(s, (0, 1))
        for s in every:
            for copy in n_sends(s, "outer") + f_sends(s, "outer"):
                copy.wait_send()

    def inner_program():
        start_n("inner")
        for copy in tables:
            copy.wait()
        z_gradient()

        def pass_on(lines, send, recv, s):
            from_outer(lines, recv, s)
            forward_copy(lines, send, recv, s).start()

        y_first(0)
        early = parts // 4
        for s in range(early):
            pass_on(n_lines, ns_sem, nr_sem, s)
        y_first(1)
        for s in range(early, parts):
            pass_on(n_lines, ns_sem, nr_sem, s)

        far_rows = chip_rows(opposite)
        for s in every:
            for j in range(2):
                landed(n_lines.at[ys(s), x_rows(opposite * 2 + j), :], nr_sem.at[2 + j, s])
        swap = to_x(mate, n_lines.at[:, far_rows, :], far_other, os_sem.at[0], or_sem.at[0])
        swap.start()

        @pl.loop(0, rows_y // 8)
        def _(j):
            y0 = pl.multiple_of(j * 8, 8)
            far_n[:, pl.ds(y0, 8), :] = jnp.swapaxes(n_lines[pl.ds(y0, 8), far_rows, :], 0, 1)

        far_send(0)
        swap.wait_recv()
        far_group = min(rows_y, max(1, 256 // chip_x))

        @pl.loop(0, rows_y // far_group)
        def _(i):
            at = pl.ds(i * far_group, far_group)
            here = n_lines[at, far_rows, :].reshape(far_group * chip_x, half)
            there = far_other[at].reshape(far_group * chip_x, half)
            result = product(here, dmz_ref[zs(core), zs(core)])
            result = result + product(there, dmz_ref[zs(1 - core), zs(core)])
            far_gz[at] = result.reshape(far_group, chip_x, half)

        def far_lines():
            far_wait(0, False)

            @pl.loop(0, far_block)
            def _(i):
                far_ry[i] = product(dmy_ref[...], far_ly[i])

            far_send(1)

        def far_pointwise(s):
            @pl.loop(0, span // step)
            def _(j):
                y0 = pl.multiple_of(s * span + j * step, step)
                far_other[pl.ds(y0, step)] = jnp.swapaxes(far_gy[:, pl.ds(y0, step), :], 0, 1)

            tall = min(32, chip_x)

            @pl.loop(0, span)
            def _(j):
                y = s * span + j

                @pl.loop(0, chip_x // tall)
                def _(i):
                    x0 = pl.multiple_of(i * tall, tall)
                    near = pl.ds(x0, tall)
                    line = pl.ds(pl.multiple_of(opposite * chip_x + x0, tall), tall)
                    dens = n_lines[y, line, :]
                    grad_x = g_lines[y, pl.ds(pl.multiple_of(first_far + x0, tall), tall), :]
                    grad_y, grad_z = far_other[y, near, :], far_gz[y, near, :]
                    grad_sq = grad_x * grad_x + grad_y * grad_y + grad_z * grad_z
                    value, pull = jax.vjp(functools.partial(xc_energy, dens), grad_sq)
                    (d_grad,) = pull(jnp.ones_like(value))
                    f_lines[y, line, :] = 2.0 * d_grad * grad_x

        for c in range(lanes_count):
            y_wait(1, c, False)
        lag = parts // 2
        for s in every:
            landed(n_lines.at[ys(s), chip_rows(far_outer), :], nr_sem.at[5, s])
            landed(n_lines.at[ys(s), x_rows(mate), :], nr_sem.at[4, s])
            x_lines(n_lines, (inner - 1) * chip_x, 3 * chip_x, s)
            x_back(first_own, first_other, gx_t, gs_sem, gr_sem, s)
            landed(gx_t.at[ys(s), :, zs(1 - core)], gr_sem.at[1 - core, s])
            pointwise(s)
            for copy in f_sends(s, "inner"):
                copy.start()
            f_lines[ys(s), x_rows(me_x), :] = fx_t[ys(s), :, zs(core)]
            if s == lag:
                far_lines()
            if s >= lag:
                pass_on(f_lines, fs_sem, fr_sem, s - lag)
        for c in range(lanes_count):
            y_send(2, c)
        energy_first()
        swap.wait_send()
        far_wait(1, False)
        for s in every:
            far_pointwise(s)
            if s < parts - lag:
                pass_on(f_lines, fs_sem, fr_sem, lag + s)
            for copy in back_copies(first_own, first_other, gx_t, gs_sem, gr_sem, s):
                copy.wait_send()
            landed(f_lines.at[ys(s), x_rows(mate), :], fr_sem.at[4, s])
            landed(f_lines.at[ys(s), chip_rows(far_outer), :], fr_sem.at[5, s])
            x_lines(f_lines, (inner - 1) * 2 * chip_x, 2 * chip_x, s)
            x_back(second_own, second_other, dx_t, ds_sem, dr_sem, s)
            if s == parts // 4:
                y_second(0)
            if s == parts // 2:
                y_second(1)
            if s == parts // 2 + 1:
                energy_second()
        z_divergence()
        energy_last()
        for c in range(lanes_count):
            y_wait(3, c, False)
        for s in every:
            finish(s, (1 - core,))
        for s in every:
            for copy in n_sends(s, "inner") + f_sends(s, "inner"):
                copy.wait_send()
            forward_copy(n_lines, ns_sem, nr_sem, s).wait_send()
            forward_copy(f_lines, fs_sem, fr_sem, s).wait_send()
            for copy in back_copies(second_own, second_other, dx_t, ds_sem, dr_sem, s):
                copy.wait_send()
        for phase in range(2):
            far_wait(phase, True)

    pl.when(is_inner)(inner_program)
    pl.when(jnp.logical_not(is_inner))(outer_program)

    for c in range(lanes_count):
        for phase in (0, 2, 3):
            y_wait(phase, c, True)
    for phase in range(2):
        for copy in energy_copies(phase):
            copy.wait_send()


def chip_body(num_gx, num_gy, density):
    rows_x, rows_y, count_z = density.shape
    count_x = rows_x * num_gx
    count_y = rows_y * num_gy
    half = count_z // 2
    parts = rows_y // 8
    span = rows_y // parts
    block_x = rows_x // num_gy
    chip_x = 2 * rows_x
    far_block = chip_x // num_gy
    straight = (rows_x, rows_y, count_z)
    turned = (rows_y, rows_x, count_z)
    lines_y = (block_x, count_y, count_z)
    deep = min(rows_x, max(1, 32 // (span * 2)))
    shapes = [
        straight, (count_x, count_x), (count_y, count_y), (count_z, count_z),
        turned, (rows_y, count_x, half), (rows_y, 3 * chip_x, half), turned, straight, turned,
        (rows_y, count_x, half), turned,
        lines_y, lines_y, lines_y, straight, straight, straight,
        (chip_x, rows_y, half), (far_block, count_y, half), (far_block, count_y, half),
        (chip_x, rows_y, half), (rows_y, chip_x, half), (rows_y, chip_x, half),
        (deep, span, count_z), (num_gy, 8, half), (8, half), (num_gx, 8, half),
    ]
    sems = [
        (4, parts), (6, parts), (3, parts), (2, parts), (4, parts), (6, parts), (3, parts), (2, parts),
        (4, 2, num_gy), (4, 2, num_gy), (2, num_gy), (2, num_gy), (1,), (1,),
        (2, num_gx), (2, num_gx), (5,),
    ]
    vmem = pl.BlockSpec(memory_space=pltpu.VMEM)
    potential, partial = pl.pallas_call(
        functools.partial(chip_kernel, num_gx, num_gy, parts),
        out_shape=(
            pltpu.VMEM(straight, jnp.float32),
            jax.ShapeDtypeStruct((1, 1), jnp.float32),
        ),
        in_specs=[pl.BlockSpec(memory_space=pltpu.HBM)] * 4,
        out_specs=(vmem, vmem),
        scratch_shapes=[pltpu.VMEM(shape, jnp.float32) for shape in shapes]
        + [pltpu.SemaphoreType.DMA(shape) for shape in sems],
        compiler_params=pltpu.CompilerParams(
            collective_id=0, has_side_effects=True, vmem_limit_bytes=67043328 - 4 * density.size - 2**16
        ),
    )(
        density,
        jnp.asarray(deriv_matrix(count_x)),
        jnp.asarray(deriv_matrix(count_y)),
        jnp.asarray(deriv_matrix(count_z).T.copy()),
    )
    return (potential, partial.reshape(()))


def body(num_gx, num_gy, density):
    rows_x, rows_y, count_z = density.shape
    count_x = rows_x * num_gx
    count_y = rows_y * num_gy
    zc = 128 if count_z % 128 == 0 else count_z
    chunks = count_z // zc
    block_y = rows_y // num_gx
    block_x = rows_x // num_gy
    straight = (rows_x, rows_y, count_z)
    turned = (rows_y, rows_x, count_z)
    lines_x = (block_y, count_x, count_z)
    lines_y = (block_x, count_y, count_z)
    shapes = [
        straight, (count_x, count_x), (count_y, count_y), (count_z, count_z),
        turned, lines_x, lines_x, turned, straight,
        lines_y, lines_y, straight, straight,
        turned, lines_x, lines_x, turned,
        lines_y, lines_y, straight,
        (min(rows_y, 32), zc), (num_gy, 8, zc), (8, zc), (num_gx, 8, zc),
    ]
    vmem = pl.BlockSpec(memory_space=pltpu.VMEM)
    potential, partial = pl.pallas_call(
        functools.partial(kernel, num_gx, num_gy, zc),
        out_shape=(
            pltpu.VMEM(straight, jnp.float32),
            jax.ShapeDtypeStruct((1, 1), jnp.float32),
        ),
        in_specs=[pl.BlockSpec(memory_space=pltpu.HBM)] * 4,
        out_specs=(vmem, vmem),
        scratch_shapes=[pltpu.VMEM(shape, jnp.float32) for shape in shapes]
        + [
            pltpu.SemaphoreType.DMA((4, chunks, num_gx)),
            pltpu.SemaphoreType.DMA((4, chunks, num_gx)),
            pltpu.SemaphoreType.DMA((4, chunks, num_gy)),
            pltpu.SemaphoreType.DMA((4, chunks, num_gy)),
            pltpu.SemaphoreType.DMA((2, num_gx)),
            pltpu.SemaphoreType.DMA((2, num_gx)),
            pltpu.SemaphoreType.DMA((chunks + 3,)),
        ],
        compiler_params=pltpu.CompilerParams(
            collective_id=0, has_side_effects=True, vmem_limit_bytes=67043328 - 4 * density.size - 2**16
        ),
    )(
        density,
        jnp.asarray(deriv_matrix(count_x)),
        jnp.asarray(deriv_matrix(count_y)),
        jnp.asarray(deriv_matrix(count_z).T.copy()),
    )
    return (potential, partial.reshape(()))


def solution(mesh):
    in_specs = (P("gx", "gy", None),)
    out_specs = (P("gx", "gy", None), P())
    num_gx, num_gy = mesh.shape["gx"], mesh.shape["gy"]

    def run(density):
        rows_x, rows_y, count_z = density.shape
        even = count_z % 256 == 0 and rows_y % 16 == 0 and rows_x % (8 * num_gy) == 0
        form = chip_body if num_gx == 8 and even else body
        return form(num_gx, num_gy, density)

    return jax.shard_map(run, mesh=mesh, in_specs=in_specs, out_specs=out_specs, check_vma=False)
```

```python
import functools
import math

import jax
import jax.numpy as jnp
import numpy as np
from jax import lax
from jax.experimental import pallas as pl
from jax.experimental.pallas import tpu as pltpu
from jax.sharding import PartitionSpec as P

spacing = 1.0
highest = lax.Precision.HIGHEST
pbe_kappa = 0.804
pbe_mu = 0.2195149727645171
pbe_beta = 0.06672455060314922
pbe_gamma = 0.031090690869654894
pw_coef = 0.0310907
pw_alpha = 0.2137
pw_first = 7.5957
pw_second = 3.5876
pw_third = 1.6382
pw_fourth = 0.49294


def xc_energy(electrons, grad_sq):
    third = jnp.exp(jnp.log(electrons) * (1.0 / 3.0))
    k_fermi = (3.0 * math.pi**2) ** (1.0 / 3.0) * third
    exch_unif = -0.75 / math.pi * k_fermi
    inv_sq = grad_sq / (4.0 * k_fermi * electrons * electrons)
    s_square = inv_sq / k_fermi
    enhance = 1.0 + pbe_kappa - pbe_kappa / (1.0 + (pbe_mu / pbe_kappa) * s_square)
    wigner = (3.0 / (4.0 * math.pi)) ** (1.0 / 3.0) / third
    root_rs = jnp.sqrt(wigner)
    series = (
        2.0
        * pw_coef
        * root_rs
        * (pw_first + root_rs * (pw_second + root_rs * (pw_third + root_rs * pw_fourth)))
    )
    corr_unif = -2.0 * pw_coef * (1.0 + pw_alpha * wigner) * jnp.log(1.0 + 1.0 / series)
    t_square = inv_sq * (math.pi / 4.0)
    factor = (pbe_beta / pbe_gamma) / (jnp.exp(corr_unif * (-1.0 / pbe_gamma)) - 1.0)
    scaled = factor * t_square
    gradient_term = pbe_gamma * jnp.log(
        1.0 + (pbe_beta / pbe_gamma) * t_square * (1.0 + scaled) / (1.0 + scaled + scaled * scaled)
    )
    return electrons * (exch_unif * enhance + corr_unif + gradient_term)


def deriv_matrix(count):
    positions = np.arange(count)
    signed = np.where(positions < count // 2, positions, positions - count)
    signed = np.where(positions == count // 2, 0, signed)
    waves = signed * (2.0 * math.pi / (count * spacing))
    phase = (positions[:, None] * positions[None, :] % count) * (2.0 * math.pi / count)
    cosine, sine = np.cos(phase), np.sin(phase)
    first = (cosine.T * waves[None, :]) @ sine
    second = (sine.T * waves[None, :]) @ cosine
    return ((first - second) / count).astype(np.float32)


def far_first(count):
    return sorted(range(1, count), key=lambda k: abs(2 * k - count))


def kernel(
    num_gx, num_gy, zc,
    n_hbm, dmx_hbm, dmy_hbm, dmz_hbm,
    out_ref, energy_ref,
    n_ref, dmx_ref, dmy_ref, dmz_ref,
    n_t, lx1, rx1, gx_t, gx, ly1, ry1, gy, gz, fx_t, lx2, rx2, dx_t, ly2, ry2, dy,
    acc, part_y, tot_y, part_x,
    xs_sem, xr_sem, ys_sem, yr_sem, es_sem, er_sem, in_sem,
):
    rows_x, rows_y, count_z = n_ref.shape
    block_y = rows_y // num_gx
    block_x = rows_x // num_gy
    count_x = rows_x * num_gx
    count_y = rows_y * num_gy
    chunks = count_z // zc
    me_x = lax.axis_index("gx")
    me_y = lax.axis_index("gy")

    def peer_x(k):
        return lax.rem(me_x + k, num_gx)

    def peer_y(k):
        return lax.rem(me_y + k, num_gy)

    def zs(c):
        return pl.ds(c * zc, zc)

    def x_block(i):
        return pl.ds(i * block_y, block_y)

    def x_rows(i):
        return pl.ds(pl.multiple_of(i * rows_x, rows_x), rows_x)

    def y_block(i):
        return pl.ds(i * block_x, block_x)

    def y_rows(i):
        return pl.ds(pl.multiple_of(i * rows_y, rows_y), rows_y)

    loads = [
        pltpu.make_async_copy(n_hbm.at[:, :, zs(c)], n_ref.at[:, :, zs(c)], in_sem.at[c])
        for c in range(chunks)
    ]
    pairs = ((dmz_hbm, dmz_ref), (dmy_hbm, dmy_ref), (dmx_hbm, dmx_ref))
    tables = [
        pltpu.make_async_copy(source, target, in_sem.at[chunks + place])
        for place, (source, target) in enumerate(pairs)
    ]
    for copy in loads + tables:
        copy.start()
    barrier = pltpu.get_barrier_semaphore()
    for k in range(1, num_gx):
        pl.semaphore_signal(
            barrier, inc=1, device_id={"gx": peer_x(k)}, device_id_type=pl.DeviceIdType.MESH
        )
    for k in range(1, num_gy):
        pl.semaphore_signal(
            barrier, inc=1, device_id={"gy": peer_y(k)}, device_id_type=pl.DeviceIdType.MESH
        )
    def send_x(phase, c, source, target, forward):
        copies = []
        for k in far_first(num_gx):
            to = peer_x(k)
            if forward:
                src, dst = source.at[x_block(to), :, zs(c)], target.at[:, x_rows(me_x), zs(c)]
            else:
                src, dst = source.at[:, x_rows(to), zs(c)], target.at[x_block(me_x), :, zs(c)]
            copy = pltpu.make_async_remote_copy(
                src_ref=src, dst_ref=dst,
                send_sem=xs_sem.at[phase, c, k], recv_sem=xr_sem.at[phase, c, k],
                device_id={"gx": to}, device_id_type=pl.DeviceIdType.MESH,
            )
            copy.start()
            copies.append(copy)
        if forward:
            target[:, x_rows(me_x), zs(c)] = source[x_block(me_x), :, zs(c)]
        else:
            target[x_block(me_x), :, zs(c)] = source[:, x_rows(me_x), zs(c)]
        return copies

    def send_y(phase, c, source, target, forward):
        copies = []
        for k in far_first(num_gy):
            to = peer_y(k)
            if forward:
                src, dst = source.at[y_block(to), :, zs(c)], target.at[:, y_rows(me_y), zs(c)]
            else:
                src, dst = source.at[:, y_rows(to), zs(c)], target.at[y_block(me_y), :, zs(c)]
            copy = pltpu.make_async_remote_copy(
                src_ref=src, dst_ref=dst,
                send_sem=ys_sem.at[phase, c, k], recv_sem=yr_sem.at[phase, c, k],
                device_id={"gy": to}, device_id_type=pl.DeviceIdType.MESH,
            )
            copy.start()
            copies.append(copy)
        if forward:
            target[:, y_rows(me_y), zs(c)] = source[y_block(me_y), :, zs(c)]
        else:
            target[y_block(me_y), :, zs(c)] = source[:, y_rows(me_y), zs(c)]
        return copies

    def arrived(copies):
        for copy in copies:
            copy.wait_recv()

    def lines(matrix, source, target, c):
        @pl.loop(0, source.shape[0])
        def _(i):
            target[i, :, zs(c)] = jnp.dot(
                matrix[...], source[i, :, zs(c)],
                precision=highest, preferred_element_type=jnp.float32,
            )

    step = min(8, rows_y)

    def turn_in(source, target, c):
        @pl.loop(0, rows_y // step)
        def _(j):
            y0 = pl.multiple_of(j * step, step)
            target[pl.ds(y0, step), :, zs(c)] = jnp.swapaxes(
                source[:, pl.ds(y0, step), zs(c)], 0, 1
            )

    def turn_out(source, target, c):
        @pl.loop(0, rows_y // step)
        def _(j):
            y0 = pl.multiple_of(j * step, step)
            target[:, pl.ds(y0, step), zs(c)] = jnp.swapaxes(
                source[pl.ds(y0, step), :, zs(c)], 0, 1
            )

    group = min(rows_x, max(1, 256 // rows_y))

    def along_z(source):
        def at(i):
            return pl.ds(i * group, group)

        def product(i):
            flat = source[at(i)].reshape(group * rows_y, count_z)
            result = jnp.dot(
                flat, dmz_ref[...], precision=highest, preferred_element_type=jnp.float32
            )
            return result.reshape(group, rows_y, count_z)

        return at, product

    sent = []
    every = range(chunks)
    fy1, fx1 = [], []
    for c in every:
        loads[c].wait()
        turn_in(n_ref, n_t, c)
        if c == 0:
            pl.semaphore_wait(barrier, num_gx + num_gy - 2)
        fx1.append(send_x(0, c, n_t, lx1, True))
        fy1.append(send_y(0, c, n_ref, ly1, True))
    for copy in tables:
        copy.wait()
    at, product = along_z(n_ref)

    @pl.loop(0, rows_x // group)
    def _(i):
        gz[at(i)] = product(i)

    by1, bx1 = [], []
    for c in every:
        arrived(fy1[c])
        lines(dmy_ref, ly1, ry1, c)
        by1.append(send_y(1, c, ry1, gy, False))
    for c in every:
        arrived(fx1[c])
        lines(dmx_ref, lx1, rx1, c)
        bx1.append(send_x(1, c, rx1, gx_t, False))

    acc[...] = jnp.zeros_like(acc)
    part = min(rows_y, 32)
    fx2, fy2 = [], []
    for c in every:
        arrived(by1[c])
        arrived(bx1[c])
        turn_out(gx_t, gx, c)

        @pl.loop(0, rows_x)
        def _(i):
            @pl.loop(0, rows_y // part)
            def _(j):
                where = (i, pl.ds(pl.multiple_of(j * part, part), part), zs(c))
                dens, grad_x, grad_y, grad_z = n_ref[where], gx[where], gy[where], gz[where]
                grad_sq = grad_x * grad_x + grad_y * grad_y + grad_z * grad_z
                value, pull = jax.vjp(xc_energy, dens, grad_sq)
                d_dens, d_grad = pull(jnp.ones_like(value))
                twice = 2.0 * d_grad
                out_ref[where] = d_dens
                gx[where] = twice * grad_x
                gy[where] = twice * grad_y
                gz[where] = twice * grad_z
                acc[...] += value

        turn_in(gx, fx_t, c)
        fx2.append(send_x(2, c, fx_t, lx2, True))
        fy2.append(send_y(2, c, gy, ly2, True))

    energy = jnp.sum(acc[...].reshape(-1, 8, zc), axis=0)
    part_y[me_y] = energy
    energy_copies = []
    for k in range(1, num_gy):
        copy = pltpu.make_async_remote_copy(
            src_ref=part_y.at[me_y], dst_ref=part_y.at[me_y],
            send_sem=es_sem.at[0, k], recv_sem=er_sem.at[0, k],
            device_id={"gy": peer_y(k)}, device_id_type=pl.DeviceIdType.MESH,
        )
        copy.start()
        energy_copies.append(copy)

    at, product = along_z(gz)

    @pl.loop(0, rows_x // group)
    def _(i):
        out_ref[at(i)] = out_ref[at(i)] - product(i)

    arrived(energy_copies)
    sent.append(energy_copies)
    tot_y[...] = jnp.sum(part_y[...], axis=0)
    part_x[me_x] = tot_y[...]
    energy_copies = []
    for k in range(1, num_gx):
        copy = pltpu.make_async_remote_copy(
            src_ref=tot_y, dst_ref=part_x.at[me_x],
            send_sem=es_sem.at[1, k], recv_sem=er_sem.at[1, k],
            device_id={"gx": peer_x(k)}, device_id_type=pl.DeviceIdType.MESH,
        )
        copy.start()
        energy_copies.append(copy)

    bx2, by2 = [], []
    for c in every:
        arrived(fy2[c])
        lines(dmy_ref, ly2, ry2, c)
        by2.append(send_y(3, c, ry2, dy, False))
        arrived(fx2[c])
        lines(dmx_ref, lx2, rx2, c)
        bx2.append(send_x(3, c, rx2, dx_t, False))

    arrived(energy_copies)
    sent.append(energy_copies)
    cells = float(count_x * count_y * count_z)
    total = jnp.sum(part_x[...], axis=0)
    energy_ref[...] = jnp.sum(total, axis=(0, 1), keepdims=True) * (1.0 / cells)

    for c in every:
        arrived(by2[c])
        arrived(bx2[c])

        @pl.loop(0, rows_y // step)
        def _(j):
            y0 = pl.multiple_of(j * step, step)
            where = (slice(None), pl.ds(y0, step), zs(c))
            turned = jnp.swapaxes(dx_t[pl.ds(y0, step), :, zs(c)], 0, 1)
            out_ref[where] = out_ref[where] - (dy[where] + turned)

    for copies in sent + fx1 + fy1 + bx1 + by1 + fx2 + fy2 + bx2 + by2:
        for copy in copies:
            copy.wait_send()


def chip_kernel(
    num_gx, num_gy, parts,
    n_hbm, dmx_hbm, dmy_hbm, dmz_hbm,
    out_ref, energy_ref,
    n_ref, dmx_ref, dmy_ref, dmz_ref,
    n_t, n_lines, g_lines, gx_t, gx, fx_t, f_lines, dx_t,
    ly1, ly2, ry, gy, dy, gz,
    far_n, far_ly, far_ry, far_gy, far_other, far_gz,
    acc, part_y, tot_y, part_x,
    ns_sem, nr_sem, gs_sem, gr_sem, fs_sem, fr_sem, ds_sem, dr_sem,
    ys_sem, yr_sem, ws_sem, wr_sem, os_sem, or_sem, es_sem, er_sem, in_sem,
):
    rows_x, rows_y, count_z = n_ref.shape
    half = count_z // 2
    chip_x = 2 * rows_x
    block_x = rows_x // num_gy
    far_block = chip_x // num_gy
    count_x = rows_x * num_gx
    count_y = rows_y * num_gy
    span = rows_y // parts
    me_x = lax.axis_index("gx")
    me_y = lax.axis_index("gy")
    core = lax.rem(me_x, 2)
    chip = me_x // 2
    chips = num_gx // 2
    is_inner = jnp.logical_and(chip > 0, chip < chips - 1)
    low = chip < 2
    inner = jnp.where(low, 1, 2)
    outer = jnp.where(low, 0, 3)
    opposite = 3 - inner
    far_outer = 3 - outer
    mate = chip * 2 + (1 - core)
    every = range(parts)
    lanes_count = 2

    def zs(c):
        if isinstance(c, int):
            return pl.ds(c * half, half)
        return pl.ds(pl.multiple_of(c * half, half), half)

    def ys(s):
        return pl.ds(s * span, span)

    def x_rows(device):
        return pl.ds(pl.multiple_of(device * rows_x, rows_x), rows_x)

    def chip_rows(which):
        return pl.ds(pl.multiple_of(which * chip_x, chip_x), chip_x)

    def local_rows(start, size):
        return pl.ds(pl.multiple_of(start, rows_x), size)

    def peer_y(k):
        return lax.rem(me_y + k, num_gy)

    def y_rows(i):
        return pl.ds(pl.multiple_of(i * rows_y, rows_y), rows_y)

    def to_x(device, source, target, send, recv):
        return pltpu.make_async_remote_copy(
            src_ref=source, dst_ref=target, send_sem=send, recv_sem=recv,
            device_id={"gx": device}, device_id_type=pl.DeviceIdType.MESH,
        )

    def landed(target, recv):
        to_x(mate, target, target, recv, recv).wait_recv()

    loads = [
        pltpu.make_async_copy(n_hbm.at[:, :, zs(c)], n_ref.at[:, :, zs(c)], in_sem.at[c])
        for c in range(lanes_count)
    ]
    pairs = ((dmz_hbm, dmz_ref), (dmy_hbm, dmy_ref), (dmx_hbm, dmx_ref))
    tables = [
        pltpu.make_async_copy(source, target, in_sem.at[lanes_count + place])
        for place, (source, target) in enumerate(pairs)
    ]
    for copy in loads + tables:
        copy.start()
    barrier = pltpu.get_barrier_semaphore()
    for k in range(1, num_gx):
        pl.semaphore_signal(
            barrier, inc=1, device_id={"gx": lax.rem(me_x + k, num_gx)},
            device_id_type=pl.DeviceIdType.MESH,
        )
    for k in range(1, num_gy):
        pl.semaphore_signal(
            barrier, inc=1, device_id={"gy": peer_y(k)}, device_id_type=pl.DeviceIdType.MESH
        )

    y_chunks = (2, 2, parts, 4)
    y_plan = ((n_ref, ly1), (ry, gy), (gy, ly2), (ry, dy))

    def y_ends(phase, c, to, mine):
        source, target = y_plan[phase]
        if phase == 2:
            line = pl.ds(pl.multiple_of(mine * rows_y + c * span, span), span)
            return source.at[pl.ds(to * block_x, block_x), ys(c)], target.at[:, line]
        rows = block_x // y_chunks[phase]
        if phase == 0:
            return (
                source.at[pl.ds(to * block_x + c * rows, rows)],
                target.at[pl.ds(c * rows, rows), y_rows(mine)],
            )
        return (
            source.at[pl.ds(c * rows, rows), y_rows(to)],
            target.at[pl.ds(mine * block_x + c * rows, rows)],
        )

    def y_copies(phase, c):
        copies = []
        for k in far_first(num_gy):
            to = peer_y(k)
            src, dst = y_ends(phase, c, to, me_y)
            copies.append(pltpu.make_async_remote_copy(
                src_ref=src, dst_ref=dst,
                send_sem=ys_sem.at[phase, c, k], recv_sem=yr_sem.at[phase, c, k],
                device_id={"gy": to}, device_id_type=pl.DeviceIdType.MESH,
            ))
        return copies

    def y_send(phase, c):
        for copy in y_copies(phase, c):
            copy.start()
        here, there = y_ends(phase, c, me_y, me_y)
        there[...] = here[...]

    def y_wait(phase, sent, chunks=None):
        for c in range(y_chunks[phase]) if chunks is None else chunks:
            for copy in y_copies(phase, c):
                if sent:
                    copy.wait_send()
                else:
                    copy.wait_recv()

    far_chunk = far_block // 2

    def far_copies(phase, h):
        copies = []
        for k in far_first(num_gy):
            to = peer_y(k)
            if phase == 0:
                src = far_n.at[pl.ds(to * far_block + h * far_chunk, far_chunk)]
                dst = far_ly.at[pl.ds(h * far_chunk, far_chunk), y_rows(me_y), :]
            else:
                src = far_ry.at[pl.ds(h * far_chunk, far_chunk), y_rows(to), :]
                dst = far_gy.at[pl.ds(me_y * far_block + h * far_chunk, far_chunk)]
            copies.append(pltpu.make_async_remote_copy(
                src_ref=src, dst_ref=dst,
                send_sem=ws_sem.at[phase, h, k], recv_sem=wr_sem.at[phase, h, k],
                device_id={"gy": to}, device_id_type=pl.DeviceIdType.MESH,
            ))
        return copies

    def far_send(phase, h):
        for copy in far_copies(phase, h):
            copy.start()
        mine = pl.ds(me_y * far_block + h * far_chunk, far_chunk)
        here = pl.ds(h * far_chunk, far_chunk)
        if phase == 0:
            far_ly[here, y_rows(me_y), :] = far_n[mine]
        else:
            far_gy[mine] = far_ry[here, y_rows(me_y), :]

    def far_wait(phase, h, sent):
        for copy in far_copies(phase, h):
            if sent:
                copy.wait_send()
            else:
                copy.wait_recv()

    def halves(values):
        high = values.astype(jnp.bfloat16)
        return high, (values - high.astype(jnp.float32)).astype(jnp.bfloat16)

    def product(left, right):
        (left_high, left_low), (right_high, right_low) = left, right
        dot = functools.partial(jnp.dot, preferred_element_type=jnp.float32)
        return dot(left_high, right_high) + (dot(left_high, right_low) + dot(left_low, right_high))

    def y_lines(source, first, last):
        @pl.loop(first, last)
        def _(i):
            ry[i] = product((dmy_ref[0], dmy_ref[1]), halves(source[i]))

    group = min(rows_x, max(1, 256 // rows_y))

    def along_z(source, i):
        flat = source[pl.ds(i * group, group)].reshape(group * rows_y, count_z)
        return product(halves(flat), (dmz_ref[0], dmz_ref[1])).reshape(group, rows_y, count_z)

    step = min(8, span)

    def turned(source, target, s):
        @pl.loop(0, span // step)
        def _(j):
            y0 = pl.multiple_of(s * span + j * step, step)
            target[pl.ds(y0, step)] = jnp.swapaxes(source[:, pl.ds(y0, step), :], 0, 1)

    def n_sends(s, role):
        copies = []
        if role == "outer":
            for j in range(2):
                copies.append(to_x(
                    inner * 2 + j, n_t.at[ys(s), :, zs(j)], n_lines.at[ys(s), x_rows(me_x), :],
                    ns_sem.at[j, s], nr_sem.at[core, s],
                ))
        else:
            for j in range(2):
                copies.append(to_x(
                    opposite * 2 + j, n_t.at[ys(s), :, zs(j)], n_lines.at[ys(s), x_rows(me_x), :],
                    ns_sem.at[j, s], nr_sem.at[2 + core, s],
                ))
            copies.append(to_x(
                mate, n_t.at[ys(s), :, zs(1 - core)], n_lines.at[ys(s), x_rows(me_x), :],
                ns_sem.at[2, s], nr_sem.at[4, s],
            ))
        return copies

    pieces = 2

    def piece(s, u):
        size = span // pieces
        return pl.ds(s * span + u * size, size)

    def forward_copies(lines, send, recv, s):
        copies = []
        for u in range(pieces):
            part = lines.at[piece(s, u), chip_rows(outer), :]
            copies.append(to_x(
                opposite * 2 + core, part, part, send.at[3 + u, s], recv.at[5 + u, s]
            ))
        return copies

    def from_outer(lines, recv, s):
        for j in range(2):
            landed(lines.at[ys(s), x_rows(outer * 2 + j), :], recv.at[j, s])

    def f_sends(s, role):
        copies = []
        if role == "outer":
            for j in range(2):
                copies.append(to_x(
                    inner * 2 + j, fx_t.at[ys(s), :, zs(j)], f_lines.at[ys(s), x_rows(me_x), :],
                    fs_sem.at[j, s], fr_sem.at[core, s],
                ))
        else:
            copies.append(to_x(
                mate, fx_t.at[ys(s), :, zs(1 - core)], f_lines.at[ys(s), x_rows(me_x), :],
                fs_sem.at[2, s], fr_sem.at[4, s],
            ))
        return copies

    def back_copies(own, other, target, send, recv, s, u=None):
        at = ys(s) if u is None else piece(s, u)
        slot = s if u is None else s * pieces + u
        copies = []
        for j in range(2):
            copies.append(to_x(
                outer * 2 + j, g_lines.at[at, local_rows(other + j * rows_x, rows_x), :],
                target.at[at, :, zs(core)], send.at[j, slot], recv.at[core, slot],
            ))
        copies.append(to_x(
            mate, g_lines.at[at, local_rows(own + (1 - core) * rows_x, rows_x), :],
            target.at[at, :, zs(core)], send.at[2, slot], recv.at[core, slot],
        ))
        return copies

    first_own, first_other, first_far = chip_x, jnp.where(low, 0, 2 * chip_x), jnp.where(low, 2 * chip_x, 0)
    second_own, second_other = jnp.where(low, chip_x, 0), jnp.where(low, 0, chip_x)

    def x_back(own, other, target, send, recv, s, u=None):
        for copy in back_copies(own, other, target, send, recv, s, u):
            copy.start()
        at = ys(s) if u is None else piece(s, u)
        target[at, :, zs(core)] = g_lines[at, local_rows(own + core * rows_x, rows_x), :]

    def x_lines(source, first_row, rows, first, count):
        @pl.loop(0, count // 2)
        def _(j):
            y = first + 2 * j
            at = pl.ds(pl.multiple_of(first_row, chip_x), rows)
            pair = jnp.concatenate([source[y], source[y + 1]], axis=1)
            result = product((dmx_ref[0, at, :], dmx_ref[1, at, :]), halves(pair))
            g_lines[y, pl.ds(0, rows), :] = result[:, :half]
            g_lines[y + 1, pl.ds(0, rows), :] = result[:, half:]

    deep = min(rows_x, max(1, 32 // (span * lanes_count)))

    def pointwise(s):
        @pl.loop(0, span // step)
        def _(j):
            y0 = pl.multiple_of(s * span + j * step, step)
            gx[:, pl.ds(y0, step), :] = jnp.swapaxes(gx_t[pl.ds(y0, step)], 0, 1)

        @pl.loop(0, rows_x // deep)
        def _(i):
            where = (pl.ds(i * deep, deep), ys(s))
            dens, grad_x, grad_y, grad_z = n_ref[where], gx[where], gy[where], gz[where]
            grad_sq = grad_x * grad_x + grad_y * grad_y + grad_z * grad_z
            value, pull = jax.vjp(xc_energy, dens, grad_sq)
            d_dens, d_grad = pull(jnp.ones_like(value))
            twice = 2.0 * d_grad
            out_ref[where] = d_dens
            gx[where] = twice * grad_x
            gy[where] = twice * grad_y
            gz[where] = twice * grad_z
            acc[...] += value

        turned(gx, fx_t, s)

    def z_gradient():
        @pl.loop(0, rows_x // group)
        def _(i):
            gz[pl.ds(i * group, group)] = along_z(n_ref, i)

    def z_divergence(first=0, last=rows_x // group):
        @pl.loop(first, last)
        def _(i):
            at = pl.ds(i * group, group)
            out_ref[at] = out_ref[at] - along_z(gz, i)

    def energy_copies(phase):
        copies = []
        count = num_gy if phase == 0 else num_gx
        for k in range(1, count):
            if phase == 0:
                to, src, dst = {"gy": peer_y(k)}, part_y.at[me_y], part_y.at[me_y]
            else:
                to, src, dst = {"gx": lax.rem(me_x + k, num_gx)}, tot_y, part_x.at[me_x]
            copies.append(pltpu.make_async_remote_copy(
                src_ref=src, dst_ref=dst,
                send_sem=es_sem.at[phase, k], recv_sem=er_sem.at[phase, k],
                device_id=to, device_id_type=pl.DeviceIdType.MESH,
            ))
        return copies

    def energy_first():
        total = jnp.sum(acc[...].reshape(-1, 8, count_z), axis=0)
        part_y[me_y] = total[:, :half] + total[:, half:]
        for copy in energy_copies(0):
            copy.start()

    def energy_second():
        for copy in energy_copies(0):
            copy.wait_recv()
        tot_y[...] = jnp.sum(part_y[...], axis=0)
        part_x[me_x] = tot_y[...]
        for copy in energy_copies(1):
            copy.start()

    def energy_last():
        for copy in energy_copies(1):
            copy.wait_recv()
        cells = float(count_x * count_y * count_z)
        total = jnp.sum(part_x[...], axis=0)
        energy_ref[...] = jnp.sum(total, axis=(0, 1), keepdims=True) * (1.0 / cells)

    def finish(s, sources):
        for u in range(pieces):
            for j in sources:
                landed(dx_t.at[piece(s, u), :, zs(j)], dr_sem.at[j, s * pieces + u])

        @pl.loop(0, span // step)
        def _(j):
            y0 = pl.multiple_of(s * span + j * step, step)
            where = (slice(None), pl.ds(y0, step))
            side = jnp.swapaxes(dx_t[pl.ds(y0, step)], 0, 1)
            out_ref[where] = out_ref[where] - (dy[where] + side)

    def start_n(role):
        for s in every:
            turned(n_ref, n_t, s)
            for copy in n_sends(s, role):
                copy.start()
            if role == "inner":
                n_lines[ys(s), x_rows(me_x), :] = n_t[ys(s), :, zs(core)]

    def y_first(c):
        rows = block_x // 2
        y_wait(0, False, (c,))
        y_lines(ly1, c * rows, (c + 1) * rows)
        y_send(1, c)

    def y_second(c):
        rows = block_x // 4
        if c == 0:
            y_wait(2, False)
            y_wait(1, True)
        y_lines(ly2, c * rows, (c + 1) * rows)
        y_send(3, c)

    acc[...] = jnp.zeros_like(acc)
    for load in loads:
        load.wait()
    pl.semaphore_wait(barrier, num_gx + num_gy - 2)
    for c in range(2):
        y_send(0, c)

    def outer_program():
        start_n("outer")
        for copy in tables:
            copy.wait()
        z_gradient()
        for c in range(2):
            y_first(c)
        y_wait(1, False)
        for s in every:
            for j in range(2):
                landed(gx_t.at[ys(s), :, zs(j)], gr_sem.at[j, s])
            pointwise(s)
            for copy in f_sends(s, "outer"):
                copy.start()
            y_send(2, s)
        energy_first()
        z_divergence()
        energy_second()
        for c in range(4):
            y_second(c)
        energy_last()
        y_wait(3, False)
        for s in every:
            finish(s, (0, 1))
        for s in every:
            for copy in n_sends(s, "outer") + f_sends(s, "outer"):
                copy.wait_send()

    def inner_program():
        start_n("inner")
        for copy in tables:
            copy.wait()
        z_gradient()

        def pass_on(lines, send, recv, s):
            from_outer(lines, recv, s)
            for copy in forward_copies(lines, send, recv, s):
                copy.start()

        far_rows = chip_rows(opposite)
        far_group = min(span, max(1, 256 // chip_x))

        def swap(s):
            return to_x(
                mate, n_lines.at[ys(s), far_rows, :], far_other.at[ys(s)], os_sem.at[s], or_sem.at[s]
            )

        def far_z(s):
            swap(s).wait_recv()

            @pl.loop(0, span // far_group)
            def _(i):
                at = pl.ds(s * span + i * far_group, far_group)
                here = n_lines[at, far_rows, :].reshape(far_group * chip_x, half)
                there = far_other[at].reshape(far_group * chip_x, half)
                table = [
                    jnp.concatenate([dmz_ref[p, zs(core), zs(core)], dmz_ref[p, zs(1 - core), zs(core)]])
                    for p in range(2)
                ]
                result = product(halves(jnp.concatenate([here, there], axis=1)), table)
                far_gz[at] = result.reshape(far_group, chip_x, half)

        for s in every:
            for j in range(2):
                landed(n_lines.at[ys(s), x_rows(opposite * 2 + j), :], nr_sem.at[2 + j, s])
            swap(s).start()

            @pl.loop(0, span // step)
            def _(j):
                y0 = pl.multiple_of(s * span + j * step, step)
                far_n[:, pl.ds(y0, step), :] = jnp.swapaxes(
                    n_lines[pl.ds(y0, step), far_rows, :], 0, 1
                )

            if s == parts - 1:
                for h in range(2):
                    far_send(0, h)
            pass_on(n_lines, ns_sem, nr_sem, s)
            if s > 0:
                far_z(s - 1)
            if s == parts // 4 - 1:
                y_first(0)
            if s == parts // 2 - 1:
                y_first(1)
        far_z(parts - 1)

        def far_lines(h):
            far_wait(0, h, False)

            @pl.loop(0, far_chunk // 2)
            def _(j):
                i = h * far_chunk + 2 * j
                pair = jnp.concatenate([far_ly[i], far_ly[i + 1]], axis=1)
                result = product((dmy_ref[0], dmy_ref[1]), halves(pair))
                far_ry[i] = result[:, :half]
                far_ry[i + 1] = result[:, half:]

            far_send(1, h)

        def far_pointwise(s):
            @pl.loop(0, span // step)
            def _(j):
                y0 = pl.multiple_of(s * span + j * step, step)
                far_other[pl.ds(y0, step)] = jnp.swapaxes(far_gy[:, pl.ds(y0, step), :], 0, 1)

            tall = min(32, chip_x)

            @pl.loop(0, span)
            def _(j):
                y = s * span + j

                @pl.loop(0, chip_x // tall)
                def _(i):
                    x0 = pl.multiple_of(i * tall, tall)
                    near = pl.ds(x0, tall)
                    line = pl.ds(pl.multiple_of(opposite * chip_x + x0, tall), tall)
                    dens = n_lines[y, line, :]
                    grad_x = g_lines[y, pl.ds(pl.multiple_of(first_far + x0, tall), tall), :]
                    grad_y, grad_z = far_other[y, near, :], far_gz[y, near, :]
                    grad_sq = grad_x * grad_x + grad_y * grad_y + grad_z * grad_z
                    value, pull = jax.vjp(functools.partial(xc_energy, dens), grad_sq)
                    (d_grad,) = pull(jnp.ones_like(value))
                    f_lines[y, line, :] = 2.0 * d_grad * grad_x

        y_wait(1, False)
        lag = parts // 2
        for s in every:
            for u in range(pieces):
                landed(n_lines.at[piece(s, u), chip_rows(far_outer), :], nr_sem.at[5 + u, s])
            landed(n_lines.at[ys(s), x_rows(mate), :], nr_sem.at[4, s])
            x_lines(n_lines, (inner - 1) * chip_x, 3 * chip_x, s * span, span)
            x_back(first_own, first_other, gx_t, gs_sem, gr_sem, s)
            landed(gx_t.at[ys(s), :, zs(1 - core)], gr_sem.at[1 - core, s])
            pointwise(s)
            for copy in f_sends(s, "inner"):
                copy.start()
            f_lines[ys(s), x_rows(me_x), :] = fx_t[ys(s), :, zs(core)]
            if s == parts // 4 - 1:
                far_lines(0)
            if s == parts // 2 - 1:
                far_lines(1)
                for ready in range(s):
                    y_send(2, ready)
            if s >= parts // 2 - 1:
                y_send(2, s)
            if s >= lag:
                pass_on(f_lines, fs_sem, fr_sem, s - lag)
        energy_first()
        for s in every:
            swap(s).wait_send()
        for h in range(2):
            far_wait(1, h, False)
        slices = rows_x // group
        for s in every:
            far_pointwise(s)
            if s < parts - lag:
                pass_on(f_lines, fs_sem, fr_sem, lag + s)
            for copy in back_copies(first_own, first_other, gx_t, gs_sem, gr_sem, s):
                copy.wait_send()
            landed(f_lines.at[ys(s), x_rows(mate), :], fr_sem.at[4, s])
            for u in range(pieces):
                landed(f_lines.at[piece(s, u), chip_rows(far_outer), :], fr_sem.at[5 + u, s])
                size = span // pieces
                x_lines(
                    f_lines, (inner - 1) * 2 * chip_x, 2 * chip_x, s * span + u * size, size
                )
                x_back(second_own, second_other, dx_t, ds_sem, dr_sem, s, u)
            z_divergence(s * slices // parts, (s + 1) * slices // parts)
            if s in (parts // 4, parts // 4 + 1):
                y_second(2 * (s - parts // 4))
                y_second(2 * (s - parts // 4) + 1)
            if s == parts // 2 + 1:
                energy_second()
        energy_last()
        y_wait(3, False)
        for s in every:
            finish(s, (1 - core,))
        for s in every:
            for copy in n_sends(s, "inner") + f_sends(s, "inner"):
                copy.wait_send()
            for copy in forward_copies(n_lines, ns_sem, nr_sem, s):
                copy.wait_send()
            for copy in forward_copies(f_lines, fs_sem, fr_sem, s):
                copy.wait_send()
            for u in range(pieces):
                for copy in back_copies(second_own, second_other, dx_t, ds_sem, dr_sem, s, u):
                    copy.wait_send()
        for phase in range(2):
            for h in range(2):
                far_wait(phase, h, True)

    pl.when(is_inner)(inner_program)
    pl.when(jnp.logical_not(is_inner))(outer_program)

    for phase in (0, 2, 3):
        y_wait(phase, True)
    for phase in range(2):
        for copy in energy_copies(phase):
            copy.wait_send()


def two_parts(matrix):
    high = matrix.astype(jnp.bfloat16)
    low = (matrix - high.astype(np.float32)).astype(jnp.bfloat16)
    return jnp.asarray(np.stack([high, low]))


def chip_body(num_gx, num_gy, density):
    rows_x, rows_y, count_z = density.shape
    count_x = rows_x * num_gx
    count_y = rows_y * num_gy
    half = count_z // 2
    parts = rows_y // 8
    span = rows_y // parts
    block_x = rows_x // num_gy
    chip_x = 2 * rows_x
    far_block = chip_x // num_gy
    straight = (rows_x, rows_y, count_z)
    turned = (rows_y, rows_x, count_z)
    lines_y = (block_x, count_y, count_z)
    deep = min(rows_x, max(1, 32 // (span * 2)))
    shapes = [
        turned, (rows_y, count_x, half), (rows_y, 3 * chip_x, half), turned, straight, turned,
        (rows_y, count_x, half), turned,
        lines_y, lines_y, lines_y, straight, straight, straight,
        (chip_x, rows_y, half), (far_block, count_y, half), (far_block, count_y, half),
        (chip_x, rows_y, half), (rows_y, chip_x, half), (rows_y, chip_x, half),
        (deep, span, count_z), (num_gy, 8, half), (8, half), (num_gx, 8, half),
    ]
    sems = [
        (5, parts), (7, parts), (3, parts), (2, parts),
        (5, parts), (7, parts), (3, 2 * parts), (2, 2 * parts),
        (4, parts, num_gy), (4, parts, num_gy), (2, 2, num_gy), (2, 2, num_gy), (parts,), (parts,),
        (2, num_gx), (2, num_gx), (5,),
    ]
    vmem = pl.BlockSpec(memory_space=pltpu.VMEM)
    potential, partial = pl.pallas_call(
        functools.partial(chip_kernel, num_gx, num_gy, parts),
        out_shape=(
            pltpu.VMEM(straight, jnp.float32),
            jax.ShapeDtypeStruct((1, 1), jnp.float32),
        ),
        in_specs=[pl.BlockSpec(memory_space=pltpu.HBM)] * 4,
        out_specs=(vmem, vmem),
        scratch_shapes=[pltpu.VMEM(straight, jnp.float32)]
        + [pltpu.VMEM((2, count, count), jnp.bfloat16) for count in (count_x, count_y, count_z)]
        + [pltpu.VMEM(shape, jnp.float32) for shape in shapes]
        + [pltpu.SemaphoreType.DMA(shape) for shape in sems],
        compiler_params=pltpu.CompilerParams(
            collective_id=0, has_side_effects=True, vmem_limit_bytes=67043328 - 4 * density.size - 2**16
        ),
    )(
        density,
        two_parts(deriv_matrix(count_x)),
        two_parts(deriv_matrix(count_y)),
        two_parts(deriv_matrix(count_z).T.copy()),
    )
    return (potential, partial.reshape(()))


def body(num_gx, num_gy, density):
    rows_x, rows_y, count_z = density.shape
    count_x = rows_x * num_gx
    count_y = rows_y * num_gy
    zc = 128 if count_z % 128 == 0 else count_z
    chunks = count_z // zc
    block_y = rows_y // num_gx
    block_x = rows_x // num_gy
    straight = (rows_x, rows_y, count_z)
    turned = (rows_y, rows_x, count_z)
    lines_x = (block_y, count_x, count_z)
    lines_y = (block_x, count_y, count_z)
    shapes = [
        straight, (count_x, count_x), (count_y, count_y), (count_z, count_z),
        turned, lines_x, lines_x, turned, straight,
        lines_y, lines_y, straight, straight,
        turned, lines_x, lines_x, turned,
        lines_y, lines_y, straight,
        (min(rows_y, 32), zc), (num_gy, 8, zc), (8, zc), (num_gx, 8, zc),
    ]
    vmem = pl.BlockSpec(memory_space=pltpu.VMEM)
    potential, partial = pl.pallas_call(
        functools.partial(kernel, num_gx, num_gy, zc),
        out_shape=(
            pltpu.VMEM(straight, jnp.float32),
            jax.ShapeDtypeStruct((1, 1), jnp.float32),
        ),
        in_specs=[pl.BlockSpec(memory_space=pltpu.HBM)] * 4,
        out_specs=(vmem, vmem),
        scratch_shapes=[pltpu.VMEM(shape, jnp.float32) for shape in shapes]
        + [
            pltpu.SemaphoreType.DMA((4, chunks, num_gx)),
            pltpu.SemaphoreType.DMA((4, chunks, num_gx)),
            pltpu.SemaphoreType.DMA((4, chunks, num_gy)),
            pltpu.SemaphoreType.DMA((4, chunks, num_gy)),
            pltpu.SemaphoreType.DMA((2, num_gx)),
            pltpu.SemaphoreType.DMA((2, num_gx)),
            pltpu.SemaphoreType.DMA((chunks + 3,)),
        ],
        compiler_params=pltpu.CompilerParams(
            collective_id=0, has_side_effects=True, vmem_limit_bytes=67043328 - 4 * density.size - 2**16
        ),
    )(
        density,
        jnp.asarray(deriv_matrix(count_x)),
        jnp.asarray(deriv_matrix(count_y)),
        jnp.asarray(deriv_matrix(count_z).T.copy()),
    )
    return (potential, partial.reshape(()))


def solution(mesh):
    in_specs = (P("gx", "gy", None),)
    out_specs = (P("gx", "gy", None), P())
    num_gx, num_gy = mesh.shape["gx"], mesh.shape["gy"]

    def run(density):
        rows_x, rows_y, count_z = density.shape
        even = count_z % 256 == 0 and rows_y % 32 == 0 and rows_x % (8 * num_gy) == 0
        form = chip_body if num_gx == 8 and even else body
        return form(num_gx, num_gy, density)

    return jax.shard_map(run, mesh=mesh, in_specs=in_specs, out_specs=out_specs, check_vma=False)
```

```python
import functools
import math

import jax
import jax.numpy as jnp
import numpy as np
from jax import lax
from jax.experimental import pallas as pl
from jax.experimental.pallas import tpu as pltpu
from jax.sharding import PartitionSpec as P

spacing = 1.0
highest = lax.Precision.HIGHEST
pbe_kappa = 0.804
pbe_mu = 0.2195149727645171
pbe_beta = 0.06672455060314922
pbe_gamma = 0.031090690869654894
pw_coef = 0.0310907
pw_alpha = 0.2137
pw_first = 7.5957
pw_second = 3.5876
pw_third = 1.6382
pw_fourth = 0.49294


def xc_energy(electrons, grad_sq):
    third = jnp.exp(jnp.log(electrons) * (1.0 / 3.0))
    k_fermi = (3.0 * math.pi**2) ** (1.0 / 3.0) * third
    exch_unif = -0.75 / math.pi * k_fermi
    inv_sq = grad_sq / (4.0 * k_fermi * electrons * electrons)
    s_square = inv_sq / k_fermi
    enhance = 1.0 + pbe_kappa - pbe_kappa / (1.0 + (pbe_mu / pbe_kappa) * s_square)
    wigner = (3.0 / (4.0 * math.pi)) ** (1.0 / 3.0) / third
    root_rs = jnp.sqrt(wigner)
    series = (
        2.0
        * pw_coef
        * root_rs
        * (pw_first + root_rs * (pw_second + root_rs * (pw_third + root_rs * pw_fourth)))
    )
    corr_unif = -2.0 * pw_coef * (1.0 + pw_alpha * wigner) * jnp.log(1.0 + 1.0 / series)
    t_square = inv_sq * (math.pi / 4.0)
    factor = (pbe_beta / pbe_gamma) / (jnp.exp(corr_unif * (-1.0 / pbe_gamma)) - 1.0)
    scaled = factor * t_square
    gradient_term = pbe_gamma * jnp.log(
        1.0 + (pbe_beta / pbe_gamma) * t_square * (1.0 + scaled) / (1.0 + scaled + scaled * scaled)
    )
    return electrons * (exch_unif * enhance + corr_unif + gradient_term)


def deriv_matrix(count):
    positions = np.arange(count)
    signed = np.where(positions < count // 2, positions, positions - count)
    signed = np.where(positions == count // 2, 0, signed)
    waves = signed * (2.0 * math.pi / (count * spacing))
    phase = (positions[:, None] * positions[None, :] % count) * (2.0 * math.pi / count)
    cosine, sine = np.cos(phase), np.sin(phase)
    first = (cosine.T * waves[None, :]) @ sine
    second = (sine.T * waves[None, :]) @ cosine
    return ((first - second) / count).astype(np.float32)


def far_first(count):
    return sorted(range(1, count), key=lambda k: abs(2 * k - count))


def kernel(
    num_gx, num_gy, zc,
    n_hbm, dmx_hbm, dmy_hbm, dmz_hbm,
    out_ref, energy_ref,
    n_ref, dmx_ref, dmy_ref, dmz_ref,
    n_t, lx1, rx1, gx_t, gx, ly1, ry1, gy, gz, fx_t, lx2, rx2, dx_t, ly2, ry2, dy,
    acc, part_y, tot_y, part_x,
    xs_sem, xr_sem, ys_sem, yr_sem, es_sem, er_sem, in_sem,
):
    rows_x, rows_y, count_z = n_ref.shape
    block_y = rows_y // num_gx
    block_x = rows_x // num_gy
    count_x = rows_x * num_gx
    count_y = rows_y * num_gy
    chunks = count_z // zc
    me_x = lax.axis_index("gx")
    me_y = lax.axis_index("gy")

    def peer_x(k):
        return lax.rem(me_x + k, num_gx)

    def peer_y(k):
        return lax.rem(me_y + k, num_gy)

    def zs(c):
        return pl.ds(c * zc, zc)

    def x_block(i):
        return pl.ds(i * block_y, block_y)

    def x_rows(i):
        return pl.ds(pl.multiple_of(i * rows_x, rows_x), rows_x)

    def y_block(i):
        return pl.ds(i * block_x, block_x)

    def y_rows(i):
        return pl.ds(pl.multiple_of(i * rows_y, rows_y), rows_y)

    loads = [
        pltpu.make_async_copy(n_hbm.at[:, :, zs(c)], n_ref.at[:, :, zs(c)], in_sem.at[c])
        for c in range(chunks)
    ]
    pairs = ((dmz_hbm, dmz_ref), (dmy_hbm, dmy_ref), (dmx_hbm, dmx_ref))
    tables = [
        pltpu.make_async_copy(source, target, in_sem.at[chunks + place])
        for place, (source, target) in enumerate(pairs)
    ]
    for copy in loads + tables:
        copy.start()
    barrier = pltpu.get_barrier_semaphore()
    for k in range(1, num_gx):
        pl.semaphore_signal(
            barrier, inc=1, device_id={"gx": peer_x(k)}, device_id_type=pl.DeviceIdType.MESH
        )
    for k in range(1, num_gy):
        pl.semaphore_signal(
            barrier, inc=1, device_id={"gy": peer_y(k)}, device_id_type=pl.DeviceIdType.MESH
        )
    def send_x(phase, c, source, target, forward):
        copies = []
        for k in far_first(num_gx):
            to = peer_x(k)
            if forward:
                src, dst = source.at[x_block(to), :, zs(c)], target.at[:, x_rows(me_x), zs(c)]
            else:
                src, dst = source.at[:, x_rows(to), zs(c)], target.at[x_block(me_x), :, zs(c)]
            copy = pltpu.make_async_remote_copy(
                src_ref=src, dst_ref=dst,
                send_sem=xs_sem.at[phase, c, k], recv_sem=xr_sem.at[phase, c, k],
                device_id={"gx": to}, device_id_type=pl.DeviceIdType.MESH,
            )
            copy.start()
            copies.append(copy)
        if forward:
            target[:, x_rows(me_x), zs(c)] = source[x_block(me_x), :, zs(c)]
        else:
            target[x_block(me_x), :, zs(c)] = source[:, x_rows(me_x), zs(c)]
        return copies

    def send_y(phase, c, source, target, forward):
        copies = []
        for k in far_first(num_gy):
            to = peer_y(k)
            if forward:
                src, dst = source.at[y_block(to), :, zs(c)], target.at[:, y_rows(me_y), zs(c)]
            else:
                src, dst = source.at[:, y_rows(to), zs(c)], target.at[y_block(me_y), :, zs(c)]
            copy = pltpu.make_async_remote_copy(
                src_ref=src, dst_ref=dst,
                send_sem=ys_sem.at[phase, c, k], recv_sem=yr_sem.at[phase, c, k],
                device_id={"gy": to}, device_id_type=pl.DeviceIdType.MESH,
            )
            copy.start()
            copies.append(copy)
        if forward:
            target[:, y_rows(me_y), zs(c)] = source[y_block(me_y), :, zs(c)]
        else:
            target[y_block(me_y), :, zs(c)] = source[:, y_rows(me_y), zs(c)]
        return copies

    def arrived(copies):
        for copy in copies:
            copy.wait_recv()

    def lines(matrix, source, target, c):
        @pl.loop(0, source.shape[0])
        def _(i):
            target[i, :, zs(c)] = jnp.dot(
                matrix[...], source[i, :, zs(c)],
                precision=highest, preferred_element_type=jnp.float32,
            )

    step = min(8, rows_y)

    def turn_in(source, target, c):
        @pl.loop(0, rows_y // step)
        def _(j):
            y0 = pl.multiple_of(j * step, step)
            target[pl.ds(y0, step), :, zs(c)] = jnp.swapaxes(
                source[:, pl.ds(y0, step), zs(c)], 0, 1
            )

    def turn_out(source, target, c):
        @pl.loop(0, rows_y // step)
        def _(j):
            y0 = pl.multiple_of(j * step, step)
            target[:, pl.ds(y0, step), zs(c)] = jnp.swapaxes(
                source[pl.ds(y0, step), :, zs(c)], 0, 1
            )

    group = min(rows_x, max(1, 256 // rows_y))

    def along_z(source):
        def at(i):
            return pl.ds(i * group, group)

        def product(i):
            flat = source[at(i)].reshape(group * rows_y, count_z)
            result = jnp.dot(
                flat, dmz_ref[...], precision=highest, preferred_element_type=jnp.float32
            )
            return result.reshape(group, rows_y, count_z)

        return at, product

    sent = []
    every = range(chunks)
    fy1, fx1 = [], []
    for c in every:
        loads[c].wait()
        turn_in(n_ref, n_t, c)
        if c == 0:
            pl.semaphore_wait(barrier, num_gx + num_gy - 2)
        fx1.append(send_x(0, c, n_t, lx1, True))
        fy1.append(send_y(0, c, n_ref, ly1, True))
    for copy in tables:
        copy.wait()
    at, product = along_z(n_ref)

    @pl.loop(0, rows_x // group)
    def _(i):
        gz[at(i)] = product(i)

    by1, bx1 = [], []
    for c in every:
        arrived(fy1[c])
        lines(dmy_ref, ly1, ry1, c)
        by1.append(send_y(1, c, ry1, gy, False))
    for c in every:
        arrived(fx1[c])
        lines(dmx_ref, lx1, rx1, c)
        bx1.append(send_x(1, c, rx1, gx_t, False))

    acc[...] = jnp.zeros_like(acc)
    part = min(rows_y, 32)
    fx2, fy2 = [], []
    for c in every:
        arrived(by1[c])
        arrived(bx1[c])
        turn_out(gx_t, gx, c)

        @pl.loop(0, rows_x)
        def _(i):
            @pl.loop(0, rows_y // part)
            def _(j):
                where = (i, pl.ds(pl.multiple_of(j * part, part), part), zs(c))
                dens, grad_x, grad_y, grad_z = n_ref[where], gx[where], gy[where], gz[where]
                grad_sq = grad_x * grad_x + grad_y * grad_y + grad_z * grad_z
                value, pull = jax.vjp(xc_energy, dens, grad_sq)
                d_dens, d_grad = pull(jnp.ones_like(value))
                twice = 2.0 * d_grad
                out_ref[where] = d_dens
                gx[where] = twice * grad_x
                gy[where] = twice * grad_y
                gz[where] = twice * grad_z
                acc[...] += value

        turn_in(gx, fx_t, c)
        fx2.append(send_x(2, c, fx_t, lx2, True))
        fy2.append(send_y(2, c, gy, ly2, True))

    energy = jnp.sum(acc[...].reshape(-1, 8, zc), axis=0)
    part_y[me_y] = energy
    energy_copies = []
    for k in range(1, num_gy):
        copy = pltpu.make_async_remote_copy(
            src_ref=part_y.at[me_y], dst_ref=part_y.at[me_y],
            send_sem=es_sem.at[0, k], recv_sem=er_sem.at[0, k],
            device_id={"gy": peer_y(k)}, device_id_type=pl.DeviceIdType.MESH,
        )
        copy.start()
        energy_copies.append(copy)

    at, product = along_z(gz)

    @pl.loop(0, rows_x // group)
    def _(i):
        out_ref[at(i)] = out_ref[at(i)] - product(i)

    arrived(energy_copies)
    sent.append(energy_copies)
    tot_y[...] = jnp.sum(part_y[...], axis=0)
    part_x[me_x] = tot_y[...]
    energy_copies = []
    for k in range(1, num_gx):
        copy = pltpu.make_async_remote_copy(
            src_ref=tot_y, dst_ref=part_x.at[me_x],
            send_sem=es_sem.at[1, k], recv_sem=er_sem.at[1, k],
            device_id={"gx": peer_x(k)}, device_id_type=pl.DeviceIdType.MESH,
        )
        copy.start()
        energy_copies.append(copy)

    bx2, by2 = [], []
    for c in every:
        arrived(fy2[c])
        lines(dmy_ref, ly2, ry2, c)
        by2.append(send_y(3, c, ry2, dy, False))
        arrived(fx2[c])
        lines(dmx_ref, lx2, rx2, c)
        bx2.append(send_x(3, c, rx2, dx_t, False))

    arrived(energy_copies)
    sent.append(energy_copies)
    cells = float(count_x * count_y * count_z)
    total = jnp.sum(part_x[...], axis=0)
    energy_ref[...] = jnp.sum(total, axis=(0, 1), keepdims=True) * (1.0 / cells)

    for c in every:
        arrived(by2[c])
        arrived(bx2[c])

        @pl.loop(0, rows_y // step)
        def _(j):
            y0 = pl.multiple_of(j * step, step)
            where = (slice(None), pl.ds(y0, step), zs(c))
            turned = jnp.swapaxes(dx_t[pl.ds(y0, step), :, zs(c)], 0, 1)
            out_ref[where] = out_ref[where] - (dy[where] + turned)

    for copies in sent + fx1 + fy1 + bx1 + by1 + fx2 + fy2 + bx2 + by2:
        for copy in copies:
            copy.wait_send()


def chip_kernel(
    num_gx, num_gy, parts,
    n_hbm, dmx_hbm, dmy_hbm, dmz_hbm,
    out_ref, energy_ref,
    n_ref, dmx_ref, dmy_ref, dmz_ref,
    n_t, n_lines, g_lines, gx_t, gx, fx_t, f_lines, dx_t,
    ly1, ly2, ry, gy, dy, gz,
    far_n, far_ly, far_ry, far_gy, far_other, far_gz,
    acc, part_y, tot_y, part_x,
    ns_sem, nr_sem, gs_sem, gr_sem, fs_sem, fr_sem, ds_sem, dr_sem,
    ys_sem, yr_sem, ws_sem, wr_sem, os_sem, or_sem, es_sem, er_sem, in_sem,
):
    rows_x, rows_y, count_z = n_ref.shape
    half = count_z // 2
    chip_x = 2 * rows_x
    block_x = rows_x // num_gy
    far_block = chip_x // num_gy
    count_x = rows_x * num_gx
    count_y = rows_y * num_gy
    span = rows_y // parts
    me_x = lax.axis_index("gx")
    me_y = lax.axis_index("gy")
    core = lax.rem(me_x, 2)
    chip = me_x // 2
    chips = num_gx // 2
    is_inner = jnp.logical_and(chip > 0, chip < chips - 1)
    low = chip < 2
    inner = jnp.where(low, 1, 2)
    outer = jnp.where(low, 0, 3)
    opposite = 3 - inner
    far_outer = 3 - outer
    mate = chip * 2 + (1 - core)
    every = range(parts)
    lanes_count = 2

    def zs(c):
        if isinstance(c, int):
            return pl.ds(c * half, half)
        return pl.ds(pl.multiple_of(c * half, half), half)

    def ys(s):
        return pl.ds(s * span, span)

    def x_rows(device):
        return pl.ds(pl.multiple_of(device * rows_x, rows_x), rows_x)

    def chip_rows(which):
        return pl.ds(pl.multiple_of(which * chip_x, chip_x), chip_x)

    def local_rows(start, size):
        return pl.ds(pl.multiple_of(start, rows_x), size)

    def peer_y(k):
        return lax.rem(me_y + k, num_gy)

    def y_rows(i):
        return pl.ds(pl.multiple_of(i * rows_y, rows_y), rows_y)

    def to_x(device, source, target, send, recv):
        return pltpu.make_async_remote_copy(
            src_ref=source, dst_ref=target, send_sem=send, recv_sem=recv,
            device_id={"gx": device}, device_id_type=pl.DeviceIdType.MESH,
        )

    def landed(target, recv):
        to_x(mate, target, target, recv, recv).wait_recv()

    loads = [
        pltpu.make_async_copy(n_hbm.at[:, :, zs(c)], n_ref.at[:, :, zs(c)], in_sem.at[c])
        for c in range(lanes_count)
    ]
    pairs = ((dmz_hbm, dmz_ref), (dmy_hbm, dmy_ref), (dmx_hbm, dmx_ref))
    tables = [
        pltpu.make_async_copy(source, target, in_sem.at[lanes_count + place])
        for place, (source, target) in enumerate(pairs)
    ]
    for copy in loads + tables:
        copy.start()
    barrier = pltpu.get_barrier_semaphore()
    for k in range(1, num_gx):
        pl.semaphore_signal(
            barrier, inc=1, device_id={"gx": lax.rem(me_x + k, num_gx)},
            device_id_type=pl.DeviceIdType.MESH,
        )
    for k in range(1, num_gy):
        pl.semaphore_signal(
            barrier, inc=1, device_id={"gy": peer_y(k)}, device_id_type=pl.DeviceIdType.MESH
        )

    y_chunks = (2, 2, parts, 4)
    y_plan = ((n_ref, ly1), (ry, gy), (gy, ly2), (ry, dy))

    def y_ends(phase, c, to, mine):
        source, target = y_plan[phase]
        if phase == 2:
            line = pl.ds(pl.multiple_of(mine * rows_y + c * span, span), span)
            return source.at[pl.ds(to * block_x, block_x), ys(c)], target.at[:, line]
        rows = block_x // y_chunks[phase]
        if phase == 0:
            return (
                source.at[pl.ds(to * block_x + c * rows, rows)],
                target.at[pl.ds(c * rows, rows), y_rows(mine)],
            )
        return (
            source.at[pl.ds(c * rows, rows), y_rows(to)],
            target.at[pl.ds(mine * block_x + c * rows, rows)],
        )

    def y_copies(phase, c):
        copies = []
        for k in far_first(num_gy):
            to = peer_y(k)
            src, dst = y_ends(phase, c, to, me_y)
            copies.append(pltpu.make_async_remote_copy(
                src_ref=src, dst_ref=dst,
                send_sem=ys_sem.at[phase, c, k], recv_sem=yr_sem.at[phase, c, k],
                device_id={"gy": to}, device_id_type=pl.DeviceIdType.MESH,
            ))
        return copies

    def y_send(phase, c):
        for copy in y_copies(phase, c):
            copy.start()
        here, there = y_ends(phase, c, me_y, me_y)
        there[...] = here[...]

    def y_wait(phase, sent, chunks=None):
        for c in range(y_chunks[phase]) if chunks is None else chunks:
            for copy in y_copies(phase, c):
                if sent:
                    copy.wait_send()
                else:
                    copy.wait_recv()

    far_chunk = far_block // 2

    def far_copies(phase, h):
        copies = []
        for k in far_first(num_gy):
            to = peer_y(k)
            if phase == 0:
                src = far_n.at[pl.ds(to * far_block + h * far_chunk, far_chunk)]
                dst = far_ly.at[pl.ds(h * far_chunk, far_chunk), y_rows(me_y), :]
            else:
                src = far_ry.at[pl.ds(h * far_chunk, far_chunk), y_rows(to), :]
                dst = far_gy.at[pl.ds(me_y * far_block + h * far_chunk, far_chunk)]
            copies.append(pltpu.make_async_remote_copy(
                src_ref=src, dst_ref=dst,
                send_sem=ws_sem.at[phase, h, k], recv_sem=wr_sem.at[phase, h, k],
                device_id={"gy": to}, device_id_type=pl.DeviceIdType.MESH,
            ))
        return copies

    def far_send(phase, h):
        for copy in far_copies(phase, h):
            copy.start()
        mine = pl.ds(me_y * far_block + h * far_chunk, far_chunk)
        here = pl.ds(h * far_chunk, far_chunk)
        if phase == 0:
            far_ly[here, y_rows(me_y), :] = far_n[mine]
        else:
            far_gy[mine] = far_ry[here, y_rows(me_y), :]

    def far_wait(phase, h, sent):
        for copy in far_copies(phase, h):
            if sent:
                copy.wait_send()
            else:
                copy.wait_recv()

    def halves(values):
        high = values.astype(jnp.bfloat16)
        return high, (values - high.astype(jnp.float32)).astype(jnp.bfloat16)

    def product(left, right):
        (left_high, left_low), (right_high, right_low) = left, right
        dot = functools.partial(jnp.dot, preferred_element_type=jnp.float32)
        return dot(left_high, right_high) + (dot(left_high, right_low) + dot(left_low, right_high))

    def y_lines(source, first, last):
        @pl.loop(first, last)
        def _(i):
            ry[i] = product((dmy_ref[0], dmy_ref[1]), halves(source[i]))

    group = min(rows_x, max(1, 256 // rows_y))

    def along_z(source, i):
        flat = source[pl.ds(i * group, group)].reshape(group * rows_y, count_z)
        return product(halves(flat), (dmz_ref[0], dmz_ref[1])).reshape(group, rows_y, count_z)

    step = min(8, span)

    def turned(source, target, s):
        @pl.loop(0, span // step)
        def _(j):
            y0 = pl.multiple_of(s * span + j * step, step)
            target[pl.ds(y0, step)] = jnp.swapaxes(source[:, pl.ds(y0, step), :], 0, 1)

    def n_sends(s, role):
        copies = []
        if role == "outer":
            for j in range(2):
                copies.append(to_x(
                    inner * 2 + j, n_t.at[ys(s), :, zs(j)], n_lines.at[ys(s), x_rows(me_x), :],
                    ns_sem.at[j, s], nr_sem.at[core, s],
                ))
        else:
            for j in range(2):
                copies.append(to_x(
                    opposite * 2 + j, n_t.at[ys(s), :, zs(j)], n_lines.at[ys(s), x_rows(me_x), :],
                    ns_sem.at[j, s], nr_sem.at[2 + core, s],
                ))
            copies.append(to_x(
                mate, n_t.at[ys(s), :, zs(1 - core)], n_lines.at[ys(s), x_rows(me_x), :],
                ns_sem.at[2, s], nr_sem.at[4, s],
            ))
        return copies

    pieces = 2

    def piece(s, u):
        size = span // pieces
        return pl.ds(s * span + u * size, size)

    def forward_copies(lines, send, recv, s):
        copies = []
        for u in range(pieces):
            part = lines.at[piece(s, u), chip_rows(outer), :]
            copies.append(to_x(
                opposite * 2 + core, part, part, send.at[3 + u, s], recv.at[5 + u, s]
            ))
        return copies

    def from_outer(lines, recv, s):
        for j in range(2):
            landed(lines.at[ys(s), x_rows(outer * 2 + j), :], recv.at[j, s])

    def f_sends(s, role):
        copies = []
        if role == "outer":
            for j in range(2):
                copies.append(to_x(
                    inner * 2 + j, fx_t.at[ys(s), :, zs(j)], f_lines.at[ys(s), x_rows(me_x), :],
                    fs_sem.at[j, s], fr_sem.at[core, s],
                ))
        else:
            copies.append(to_x(
                mate, fx_t.at[ys(s), :, zs(1 - core)], f_lines.at[ys(s), x_rows(me_x), :],
                fs_sem.at[2, s], fr_sem.at[4, s],
            ))
        return copies

    def back_copies(own, other, target, send, recv, s, u=None):
        at = ys(s) if u is None else piece(s, u)
        slot = s if u is None else s * pieces + u
        copies = []
        for j in range(2):
            copies.append(to_x(
                outer * 2 + j, g_lines.at[at, local_rows(other + j * rows_x, rows_x), :],
                target.at[at, :, zs(core)], send.at[j, slot], recv.at[core, slot],
            ))
        copies.append(to_x(
            mate, g_lines.at[at, local_rows(own + (1 - core) * rows_x, rows_x), :],
            target.at[at, :, zs(core)], send.at[2, slot], recv.at[core, slot],
        ))
        return copies

    first_own, first_other, first_far = chip_x, jnp.where(low, 0, 2 * chip_x), jnp.where(low, 2 * chip_x, 0)
    second_own, second_other = jnp.where(low, chip_x, 0), jnp.where(low, 0, chip_x)

    def x_back(own, other, target, send, recv, s, u=None):
        for copy in back_copies(own, other, target, send, recv, s, u):
            copy.start()
        at = ys(s) if u is None else piece(s, u)
        target[at, :, zs(core)] = g_lines[at, local_rows(own + core * rows_x, rows_x), :]

    def x_lines(source, first_row, rows, first, count):
        @pl.loop(0, count // 2)
        def _(j):
            y = first + 2 * j
            at = pl.ds(pl.multiple_of(first_row, chip_x), rows)
            pair = jnp.concatenate([source[y], source[y + 1]], axis=1)
            result = product((dmx_ref[0, at, :], dmx_ref[1, at, :]), halves(pair))
            g_lines[y, pl.ds(0, rows), :] = result[:, :half]
            g_lines[y + 1, pl.ds(0, rows), :] = result[:, half:]

    deep = min(rows_x, max(1, 32 // (span * lanes_count)))

    def pointwise(s):
        @pl.loop(0, span // step)
        def _(j):
            y0 = pl.multiple_of(s * span + j * step, step)
            gx[:, pl.ds(y0, step), :] = jnp.swapaxes(gx_t[pl.ds(y0, step)], 0, 1)

        @pl.loop(0, rows_x // deep)
        def _(i):
            where = (pl.ds(i * deep, deep), ys(s))
            dens, grad_x, grad_y, grad_z = n_ref[where], gx[where], gy[where], gz[where]
            grad_sq = grad_x * grad_x + grad_y * grad_y + grad_z * grad_z
            value, pull = jax.vjp(xc_energy, dens, grad_sq)
            d_dens, d_grad = pull(jnp.ones_like(value))
            twice = 2.0 * d_grad
            out_ref[where] = d_dens
            gx[where] = twice * grad_x
            gy[where] = twice * grad_y
            gz[where] = twice * grad_z
            acc[...] += value

        turned(gx, fx_t, s)

    def z_gradient():
        @pl.loop(0, rows_x // group)
        def _(i):
            gz[pl.ds(i * group, group)] = along_z(n_ref, i)

    def z_divergence(first=0, last=rows_x // group):
        @pl.loop(first, last)
        def _(i):
            at = pl.ds(i * group, group)
            out_ref[at] = out_ref[at] - along_z(gz, i)

    def energy_copies(phase):
        copies = []
        count = num_gy if phase == 0 else num_gx
        for k in range(1, count):
            if phase == 0:
                to, src, dst = {"gy": peer_y(k)}, part_y.at[me_y], part_y.at[me_y]
            else:
                to, src, dst = {"gx": lax.rem(me_x + k, num_gx)}, tot_y, part_x.at[me_x]
            copies.append(pltpu.make_async_remote_copy(
                src_ref=src, dst_ref=dst,
                send_sem=es_sem.at[phase, k], recv_sem=er_sem.at[phase, k],
                device_id=to, device_id_type=pl.DeviceIdType.MESH,
            ))
        return copies

    def energy_first():
        total = jnp.sum(acc[...].reshape(-1, 8, count_z), axis=0)
        part_y[me_y] = total[:, :half] + total[:, half:]
        for copy in energy_copies(0):
            copy.start()

    def energy_second():
        for copy in energy_copies(0):
            copy.wait_recv()
        tot_y[...] = jnp.sum(part_y[...], axis=0)
        part_x[me_x] = tot_y[...]
        for copy in energy_copies(1):
            copy.start()

    def energy_last():
        for copy in energy_copies(1):
            copy.wait_recv()
        cells = float(count_x * count_y * count_z)
        total = jnp.sum(part_x[...], axis=0)
        energy_ref[...] = jnp.sum(total, axis=(0, 1), keepdims=True) * (1.0 / cells)

    def finish(s, sources):
        for u in range(pieces):
            for j in sources:
                landed(dx_t.at[piece(s, u), :, zs(j)], dr_sem.at[j, s * pieces + u])

        @pl.loop(0, span // step)
        def _(j):
            y0 = pl.multiple_of(s * span + j * step, step)
            where = (slice(None), pl.ds(y0, step))
            side = jnp.swapaxes(dx_t[pl.ds(y0, step)], 0, 1)
            out_ref[where] = out_ref[where] - (dy[where] + side)

    def start_n(role):
        for s in every:
            turned(n_ref, n_t, s)
            for copy in n_sends(s, role):
                copy.start()
            if role == "inner":
                n_lines[ys(s), x_rows(me_x), :] = n_t[ys(s), :, zs(core)]

    def y_first(c):
        rows = block_x // 2
        y_wait(0, False, (c,))
        y_lines(ly1, c * rows, (c + 1) * rows)
        y_send(1, c)

    def y_second(c):
        rows = block_x // 4
        if c == 0:
            y_wait(2, False)
            y_wait(1, True)
        y_lines(ly2, c * rows, (c + 1) * rows)
        y_send(3, c)

    acc[...] = jnp.zeros_like(acc)
    for load in loads:
        load.wait()
    pl.semaphore_wait(barrier, num_gx + num_gy - 2)
    for c in range(2):
        y_send(0, c)

    def outer_program():
        start_n("outer")
        for copy in tables:
            copy.wait()
        z_gradient()
        for c in range(2):
            y_first(c)
        y_wait(1, False)
        for s in every:
            for j in range(2):
                landed(gx_t.at[ys(s), :, zs(j)], gr_sem.at[j, s])
            pointwise(s)
            for copy in f_sends(s, "outer"):
                copy.start()
            y_send(2, s)
        energy_first()
        for c in range(4):
            y_second(c)
        energy_second()
        z_divergence()
        energy_last()
        y_wait(3, False)
        for s in every:
            finish(s, (0, 1))
        for s in every:
            for copy in n_sends(s, "outer") + f_sends(s, "outer"):
                copy.wait_send()

    def inner_program():
        start_n("inner")
        for copy in tables:
            copy.wait()
        z_gradient()

        def pass_on(lines, send, recv, s):
            from_outer(lines, recv, s)
            for copy in forward_copies(lines, send, recv, s):
                copy.start()

        far_rows = chip_rows(opposite)
        far_group = min(span, max(1, 256 // chip_x))

        def swap(s):
            return to_x(
                mate, n_lines.at[ys(s), far_rows, :], far_other.at[ys(s)], os_sem.at[s], or_sem.at[s]
            )

        def far_z(s):
            swap(s).wait_recv()

            @pl.loop(0, span // far_group)
            def _(i):
                at = pl.ds(s * span + i * far_group, far_group)
                here = n_lines[at, far_rows, :].reshape(far_group * chip_x, half)
                there = far_other[at].reshape(far_group * chip_x, half)
                table = [
                    jnp.concatenate([dmz_ref[p, zs(core), zs(core)], dmz_ref[p, zs(1 - core), zs(core)]])
                    for p in range(2)
                ]
                result = product(halves(jnp.concatenate([here, there], axis=1)), table)
                far_gz[at] = result.reshape(far_group, chip_x, half)

        for s in every:
            for j in range(2):
                landed(n_lines.at[ys(s), x_rows(opposite * 2 + j), :], nr_sem.at[2 + j, s])
            swap(s).start()

            @pl.loop(0, span // step)
            def _(j):
                y0 = pl.multiple_of(s * span + j * step, step)
                far_n[:, pl.ds(y0, step), :] = jnp.swapaxes(
                    n_lines[pl.ds(y0, step), far_rows, :], 0, 1
                )

            if s == parts - 1:
                for h in range(2):
                    far_send(0, h)
            pass_on(n_lines, ns_sem, nr_sem, s)
            if s > 0:
                far_z(s - 1)
            if s == parts // 4 - 1:
                y_first(0)
            if s == parts // 2 - 1:
                y_first(1)
        far_z(parts - 1)

        def far_lines(h):
            far_wait(0, h, False)

            @pl.loop(0, far_chunk // 2)
            def _(j):
                i = h * far_chunk + 2 * j
                pair = jnp.concatenate([far_ly[i], far_ly[i + 1]], axis=1)
                result = product((dmy_ref[0], dmy_ref[1]), halves(pair))
                far_ry[i] = result[:, :half]
                far_ry[i + 1] = result[:, half:]

            far_send(1, h)

        def far_pointwise(s):
            @pl.loop(0, span // step)
            def _(j):
                y0 = pl.multiple_of(s * span + j * step, step)
                far_other[pl.ds(y0, step)] = jnp.swapaxes(far_gy[:, pl.ds(y0, step), :], 0, 1)

            tall = min(32, chip_x)

            @pl.loop(0, span)
            def _(j):
                y = s * span + j

                @pl.loop(0, chip_x // tall)
                def _(i):
                    x0 = pl.multiple_of(i * tall, tall)
                    near = pl.ds(x0, tall)
                    line = pl.ds(pl.multiple_of(opposite * chip_x + x0, tall), tall)
                    dens = n_lines[y, line, :]
                    grad_x = g_lines[y, pl.ds(pl.multiple_of(first_far + x0, tall), tall), :]
                    grad_y, grad_z = far_other[y, near, :], far_gz[y, near, :]
                    grad_sq = grad_x * grad_x + grad_y * grad_y + grad_z * grad_z
                    value, pull = jax.vjp(functools.partial(xc_energy, dens), grad_sq)
                    (d_grad,) = pull(jnp.ones_like(value))
                    f_lines[y, line, :] = 2.0 * d_grad * grad_x

        y_wait(1, False)
        lag = parts // 2
        slices = rows_x // group

        def far_step(s):
            far_pointwise(s)
            if s < parts - lag:
                pass_on(f_lines, fs_sem, fr_sem, lag + s)
            for copy in back_copies(first_own, first_other, gx_t, gs_sem, gr_sem, s):
                copy.wait_send()
            landed(f_lines.at[ys(s), x_rows(mate), :], fr_sem.at[4, s])
            for u in range(pieces):
                landed(f_lines.at[piece(s, u), chip_rows(far_outer), :], fr_sem.at[5 + u, s])
                size = span // pieces
                x_lines(
                    f_lines, (inner - 1) * 2 * chip_x, 2 * chip_x, s * span + u * size, size
                )
                x_back(second_own, second_other, dx_t, ds_sem, dr_sem, s, u)

        for s in every:
            landed(n_lines.at[ys(s), x_rows(mate), :], nr_sem.at[4, s])
            for u in range(pieces):
                landed(n_lines.at[piece(s, u), chip_rows(far_outer), :], nr_sem.at[5 + u, s])
            x_lines(n_lines, (inner - 1) * chip_x, 3 * chip_x, s * span, span)
            x_back(first_own, first_other, gx_t, gs_sem, gr_sem, s)
            if s == parts - 1:
                pass_on(f_lines, fs_sem, fr_sem, s - lag)
                for other in every:
                    swap(other).wait_send()
                for h in range(2):
                    far_wait(1, h, False)
                far_step(0)
            landed(gx_t.at[ys(s), :, zs(1 - core)], gr_sem.at[1 - core, s])
            pointwise(s)
            for copy in f_sends(s, "inner"):
                copy.start()
            f_lines[ys(s), x_rows(me_x), :] = fx_t[ys(s), :, zs(core)]
            if s == parts // 4 - 1:
                far_lines(0)
            if s == parts // 2 - 1:
                far_lines(1)
                for ready in range(s):
                    y_send(2, ready)
            if s >= parts // 2 - 1:
                y_send(2, s)
            if lag <= s < parts - 1:
                pass_on(f_lines, fs_sem, fr_sem, s - lag)
        energy_first()
        for s in every:
            if s > 0:
                far_step(s)
            z_divergence(s * slices // parts, (s + 1) * slices // parts)
            if s in (parts // 4, parts // 4 + 1):
                y_second(2 * (s - parts // 4))
                y_second(2 * (s - parts // 4) + 1)
            if s == parts // 2 + 1:
                energy_second()
        energy_last()
        y_wait(3, False)
        for s in every:
            finish(s, (1 - core,))
        for s in every:
            for copy in n_sends(s, "inner") + f_sends(s, "inner"):
                copy.wait_send()
            for copy in forward_copies(n_lines, ns_sem, nr_sem, s):
                copy.wait_send()
            for copy in forward_copies(f_lines, fs_sem, fr_sem, s):
                copy.wait_send()
            for u in range(pieces):
                for copy in back_copies(second_own, second_other, dx_t, ds_sem, dr_sem, s, u):
                    copy.wait_send()
        for phase in range(2):
            for h in range(2):
                far_wait(phase, h, True)

    pl.when(is_inner)(inner_program)
    pl.when(jnp.logical_not(is_inner))(outer_program)

    for phase in (0, 2, 3):
        y_wait(phase, True)
    for phase in range(2):
        for copy in energy_copies(phase):
            copy.wait_send()


def two_parts(matrix):
    high = matrix.astype(jnp.bfloat16)
    low = (matrix - high.astype(np.float32)).astype(jnp.bfloat16)
    return jnp.asarray(np.stack([high, low]))


def chip_body(num_gx, num_gy, density):
    rows_x, rows_y, count_z = density.shape
    count_x = rows_x * num_gx
    count_y = rows_y * num_gy
    half = count_z // 2
    parts = rows_y // 8
    span = rows_y // parts
    block_x = rows_x // num_gy
    chip_x = 2 * rows_x
    far_block = chip_x // num_gy
    straight = (rows_x, rows_y, count_z)
    turned = (rows_y, rows_x, count_z)
    lines_y = (block_x, count_y, count_z)
    deep = min(rows_x, max(1, 32 // (span * 2)))
    shapes = [
        turned, (rows_y, count_x, half), (rows_y, 3 * chip_x, half), turned, straight, turned,
        (rows_y, count_x, half), turned,
        lines_y, lines_y, lines_y, straight, straight, straight,
        (chip_x, rows_y, half), (far_block, count_y, half), (far_block, count_y, half),
        (chip_x, rows_y, half), (rows_y, chip_x, half), (rows_y, chip_x, half),
        (deep, span, count_z), (num_gy, 8, half), (8, half), (num_gx, 8, half),
    ]
    sems = [
        (5, parts), (7, parts), (3, parts), (2, parts),
        (5, parts), (7, parts), (3, 2 * parts), (2, 2 * parts),
        (4, parts, num_gy), (4, parts, num_gy), (2, 2, num_gy), (2, 2, num_gy), (parts,), (parts,),
        (2, num_gx), (2, num_gx), (5,),
    ]
    vmem = pl.BlockSpec(memory_space=pltpu.VMEM)
    potential, partial = pl.pallas_call(
        functools.partial(chip_kernel, num_gx, num_gy, parts),
        out_shape=(
            pltpu.VMEM(straight, jnp.float32),
            jax.ShapeDtypeStruct((1, 1), jnp.float32),
        ),
        in_specs=[pl.BlockSpec(memory_space=pltpu.HBM)] * 4,
        out_specs=(vmem, vmem),
        scratch_shapes=[pltpu.VMEM(straight, jnp.float32)]
        + [pltpu.VMEM((2, count, count), jnp.bfloat16) for count in (count_x, count_y, count_z)]
        + [pltpu.VMEM(shape, jnp.float32) for shape in shapes]
        + [pltpu.SemaphoreType.DMA(shape) for shape in sems],
        compiler_params=pltpu.CompilerParams(
            collective_id=0, has_side_effects=True, vmem_limit_bytes=67043328 - 4 * density.size - 2**16
        ),
    )(
        density,
        two_parts(deriv_matrix(count_x)),
        two_parts(deriv_matrix(count_y)),
        two_parts(deriv_matrix(count_z).T.copy()),
    )
    return (potential, partial.reshape(()))


def body(num_gx, num_gy, density):
    rows_x, rows_y, count_z = density.shape
    count_x = rows_x * num_gx
    count_y = rows_y * num_gy
    zc = 128 if count_z % 128 == 0 else count_z
    chunks = count_z // zc
    block_y = rows_y // num_gx
    block_x = rows_x // num_gy
    straight = (rows_x, rows_y, count_z)
    turned = (rows_y, rows_x, count_z)
    lines_x = (block_y, count_x, count_z)
    lines_y = (block_x, count_y, count_z)
    shapes = [
        straight, (count_x, count_x), (count_y, count_y), (count_z, count_z),
        turned, lines_x, lines_x, turned, straight,
        lines_y, lines_y, straight, straight,
        turned, lines_x, lines_x, turned,
        lines_y, lines_y, straight,
        (min(rows_y, 32), zc), (num_gy, 8, zc), (8, zc), (num_gx, 8, zc),
    ]
    vmem = pl.BlockSpec(memory_space=pltpu.VMEM)
    potential, partial = pl.pallas_call(
        functools.partial(kernel, num_gx, num_gy, zc),
        out_shape=(
            pltpu.VMEM(straight, jnp.float32),
            jax.ShapeDtypeStruct((1, 1), jnp.float32),
        ),
        in_specs=[pl.BlockSpec(memory_space=pltpu.HBM)] * 4,
        out_specs=(vmem, vmem),
        scratch_shapes=[pltpu.VMEM(shape, jnp.float32) for shape in shapes]
        + [
            pltpu.SemaphoreType.DMA((4, chunks, num_gx)),
            pltpu.SemaphoreType.DMA((4, chunks, num_gx)),
            pltpu.SemaphoreType.DMA((4, chunks, num_gy)),
            pltpu.SemaphoreType.DMA((4, chunks, num_gy)),
            pltpu.SemaphoreType.DMA((2, num_gx)),
            pltpu.SemaphoreType.DMA((2, num_gx)),
            pltpu.SemaphoreType.DMA((chunks + 3,)),
        ],
        compiler_params=pltpu.CompilerParams(
            collective_id=0, has_side_effects=True, vmem_limit_bytes=67043328 - 4 * density.size - 2**16
        ),
    )(
        density,
        jnp.asarray(deriv_matrix(count_x)),
        jnp.asarray(deriv_matrix(count_y)),
        jnp.asarray(deriv_matrix(count_z).T.copy()),
    )
    return (potential, partial.reshape(()))


def solution(mesh):
    in_specs = (P("gx", "gy", None),)
    out_specs = (P("gx", "gy", None), P())
    num_gx, num_gy = mesh.shape["gx"], mesh.shape["gy"]

    def run(density):
        rows_x, rows_y, count_z = density.shape
        even = count_z % 256 == 0 and rows_y % 32 == 0 and rows_x % (8 * num_gy) == 0
        form = chip_body if num_gx == 8 and even else body
        return form(num_gx, num_gy, density)

    return jax.shard_map(run, mesh=mesh, in_specs=in_specs, out_specs=out_specs, check_vma=False)
```
